1024 devices in a mesh: panel: 8 (over y), tile: 32 (over z, core), lev: 4 (over x).
Axes of the slice: x: 4, y: 8, z: 16, core: 2. Of those that a mesh axis runs over, the one named last changes fastest.
Arguments:
- adjoint_new: float32 [5, 32, 524288], P(None, 'lev', ('panel', 'tile')), may hold values from -6 to 6
- weights: float32 [4, 524288], P(None, ('panel', 'tile', 'lev')), may hold values from 0.05 to 0.5
- departure: int32 [4, 524288], P(None, ('panel', 'tile')), may hold values from 0 to 2047
- send_point: int32 [4, 32768], P(None, ('panel', 'tile')), may hold values from 0 to 8191, as said below
- block_count: int32 [4, 256], P(None, ('panel', 'tile')), may hold values from 0 to 128, as said below
- rotation: int32 [2, 256], P(None, ('panel', 'tile')), may hold values from 0 to 3
Outputs:
- adjoint_old: float32 [5, 32, 524288], P(None, 'lev', ('panel', 'tile'))
The draws below stay inside these ranges and needn't reach their ends.
Inputs may be any that keep to these rules, and one draw needn't show every extreme that they name: `send_point`: within one tile the 512 entries are distinct stencil point numbers k * 2048 + c of that tile's own cells. `block_count`: zero for block 0 on the first tile and for block 1 on the last tile of each sector; every block position reaches 128 on some tile in every draw.
All inputs are finite; a program needn't handle non-finite values.
Results may differ from the reference program's by a relative error of at most 0.00002.
Values sent between devices are 32-bit elements; how exact they have to be, the bound alone decides.
A program may use at most 32 MiB of HBM per device.

```python
import jax
import jax.numpy as jnp
from jax import lax

FIELDS = 5
STENCIL = 4
SLOTS = 128
CELLS_DEV = 2048
CELLS = 524288
LEVELS = 32
N_PANEL = 8
N_TILE = 32


def draw_send_point(key, part):
    devices = N_PANEL * N_TILE
    keys = jax.random.split(jax.random.fold_in(key, 11), devices)

    def one_tile(tile_key):
        order = jax.random.permutation(tile_key, STENCIL * CELLS_DEV)
        return order[:4 * SLOTS].reshape(4, SLOTS)
    picks = jax.vmap(one_tile)(keys)
    return jnp.transpose(picks, (1, 0, 2)).reshape(4, devices * SLOTS).astype(jnp.int32)


def draw_block_count(key, part):
    devices = N_PANEL * N_TILE
    base_key = jax.random.fold_in(key, 23)
    key_low, key_high, key_busy, key_panel, key_tile = jax.random.split(base_key, 5)
    low_count = jax.random.randint(key_low, (4, devices), SLOTS // 8, SLOTS // 2 + 1)
    high_count = jax.random.randint(key_high, (4, devices), 3 * SLOTS // 4, SLOTS + 1)
    busy_tile = jax.random.randint(key_busy, (4, devices), 0, 8) == 0
    counts = jnp.where(busy_tile, high_count, low_count)
    device = jnp.arange(devices, dtype=jnp.int32)
    panel_of = device // N_TILE
    tile_of = device % N_TILE
    pick_panel = jax.random.randint(key_panel, (4,), 0, N_PANEL)
    pick_tile = jax.random.randint(key_tile, (4,), 1, N_TILE - 1)
    full_tile = (panel_of[None, :] == pick_panel[:, None]) & (tile_of[None, :] == pick_tile[:, None])
    counts = jnp.where(full_tile, SLOTS, counts)
    edge_zero = jnp.stack([tile_of == 0, tile_of == N_TILE - 1, tile_of < 0, tile_of < 0])
    counts = jnp.where(edge_zero, 0, counts)
    return counts.astype(jnp.int32)


def touch_ends(drawn, stream_key, low, largest):
    dims = drawn.shape
    place = [jax.random.randint(jax.random.fold_in(stream_key, axis), (), 0, dims[axis]) for axis in range(len(dims))]
    drawn = drawn.at[tuple(place)].set(low)
    longest = dims.index(max(dims))
    place[longest] = (place[longest] + 1) % dims[longest]
    return drawn.at[tuple(place)].set(largest)


def block_levels(own_key, extent, shards, least, largest):
    loudness = 1.0
    for dim, parts in shards:
        steps = jax.random.uniform(jax.random.fold_in(jax.random.fold_in(own_key, 6), dim), (parts,), jnp.float32, least / len(shards), largest / len(shards))
        loudness = loudness * jnp.repeat(jnp.exp(steps), extent[dim] // parts).reshape((-1,) + (1,) * (len(extent) - 1 - dim))
    return loudness


def scatter_about(key, dims, deviation, bound, pieces=(), kind=jnp.bfloat16):
    result = jax.random.normal(key, dims, jnp.float32) * deviation
    if len(pieces) > 0:
        result = block_levels(key, dims, pieces, -0.22, 0.18) * result
    return jnp.clip(result, min=-bound, max=bound).astype(kind)


def setup_inputs(seed: int = 0) -> dict:
    streams_of = jax.random.split(jax.random.key(seed), 7)
    return {
        "adjoint_new": scatter_about(streams_of[0], (FIELDS, LEVELS, CELLS), 1.0, 6.0, ((1, 4), (2, 256)), jnp.float32),
        "weights": jnp.clip(0.05 + 0.45 * jax.random.uniform(streams_of[1], (STENCIL, CELLS), jnp.float32) ** block_levels(streams_of[1], (STENCIL, CELLS), ((1, 1024),), -0.2, 0.2), 0.05, 0.5),
        "departure": touch_ends(jax.random.randint(streams_of[2], (STENCIL, CELLS), 0, CELLS_DEV), jax.random.fold_in(streams_of[2], 1), 0, CELLS_DEV - 1).astype(jnp.int32),
        "send_point": draw_send_point(jax.random.fold_in(streams_of[6], 71), 0),
        "block_count": draw_block_count(jax.random.fold_in(streams_of[6], 71), 0),
        "rotation": touch_ends(jax.random.randint(streams_of[5], (2, N_PANEL * N_TILE), 0, 4), jax.random.fold_in(streams_of[5], 1), 0, 3).astype(jnp.int32),
    }


def routing(departure, send_point, block_count, rotation):
    devices = N_PANEL * N_TILE
    points = STENCIL * CELLS
    column = jnp.arange(CELLS, dtype=jnp.int32)
    home_base = (column // CELLS_DEV) * CELLS_DEV
    target = (home_base[None, :] + departure).reshape(-1)
    device = jnp.arange(devices, dtype=jnp.int32)
    panel_of = device // N_TILE
    tile_of = device % N_TILE
    owners = jnp.stack([panel_of * N_TILE + tile_of - 1, panel_of * N_TILE + tile_of + 1, ((panel_of + N_PANEL - 1) % N_PANEL) * N_TILE + tile_of, ((panel_of + 1) % N_PANEL) * N_TILE + tile_of])
    chosen = send_point.reshape(4, devices, SLOTS)
    stencil_row = chosen // CELLS_DEV
    cell_col = device[None, :, None] * CELLS_DEV + chosen % CELLS_DEV
    landing = departure[stencil_row, cell_col]
    sent_target = owners[:, :, None] * CELLS_DEV + landing
    live_mask = jnp.arange(SLOTS, dtype=jnp.int32)[None, None, :] < block_count[:, :, None]
    flat_slot = jnp.where(live_mask, stencil_row * CELLS + cell_col, points).reshape(-1)
    target = target.at[flat_slot].set(sent_target.reshape(-1), mode="drop")
    turn_rows = jnp.concatenate([jnp.zeros((2, devices), jnp.int32), rotation], axis=0)
    spread_turn = jnp.broadcast_to(turn_rows[:, :, None], (4, devices, SLOTS)).reshape(-1)
    turn_code = jnp.zeros((points,), jnp.int32).at[flat_slot].set(spread_turn, mode="drop")
    return target.reshape(STENCIL, CELLS), turn_code.reshape(STENCIL, CELLS)


def reference(adjoint_new, weights, departure, send_point, block_count, rotation):
    target, turn_code = routing(departure, send_point, block_count, rotation)
    by_cell = jnp.transpose(adjoint_new, (2, 0, 1))
    cosine = (turn_code == 0).astype(jnp.float32) - (turn_code == 2).astype(jnp.float32)
    sine_term = (turn_code == 1).astype(jnp.float32) - (turn_code == 3).astype(jnp.float32)

    def one_point(summed, point_k):
        cosine_k = cosine[point_k][:, None]
        sine_k = sine_term[point_k][:, None]
        zonal_part = by_cell[:, 0, :]
        merid_part = by_cell[:, 1, :]
        turned = jnp.concatenate([(cosine_k * zonal_part + sine_k * merid_part)[:, None, :], (cosine_k * merid_part - sine_k * zonal_part)[:, None, :], by_cell[:, 2:, :]], axis=1)
        turned = turned * weights[point_k][:, None, None]
        return summed.at[target[point_k]].add(turned), None

    summed, _ = lax.scan(one_point, jnp.zeros(by_cell.shape, adjoint_new.dtype), jnp.arange(STENCIL, dtype=jnp.int32))
    return jnp.transpose(summed, (1, 2, 0))
```

```python
import functools

import jax
import jax.numpy as jnp
from jax import lax
from jax.experimental import pallas as pl
from jax.experimental.pallas import tpu as pltpu
from jax.sharding import PartitionSpec as P

MESH = pl.DeviceIdType.MESH
LOW = 256
F32, BF16, I32 = jnp.float32, jnp.bfloat16, jnp.int32


def split_rows(value):
    high = value.astype(BF16).astype(F32)
    return jnp.concatenate([high, value - high], axis=0).astype(BF16)


def one_hot(low, columns):
    rows = lax.broadcasted_iota(I32, (LOW, columns), 0)
    return jnp.where(rows == low, 1.0, 0.0).astype(BF16)


def times_transposed(lhs, rhs):
    return lax.dot_general(lhs, rhs, (((1,), (1,)), ((), ())), preferred_element_type=F32)


def spread(value, target_high, target_low, groups):
    parts = split_rows(value)
    copies = parts.shape[0] // 16
    high = jnp.broadcast_to(target_high, (16, LOW))
    lhs = []
    for g in range(groups):
        mask = jnp.where(high == g, 1.0, 0.0).astype(BF16)
        lhs.append(parts * jnp.concatenate([mask] * copies, axis=0))
    return times_transposed(jnp.concatenate(lhs, axis=0), one_hot(target_low, LOW))


def kernel(
    sizes,
    x_hbm,
    w_hbm,
    dep_hbm,
    sp_hbm,
    count_ref,
    turn_ref,
    out_ref,
    x,
    w,
    dep,
    sp,
    hot,
    glhs,
    sent,
    picked,
    acc,
    pay,
    recv,
    in_sem,
    w_send,
    w_recv,
    p_send,
    p_recv,
):
    n_panel, n_tile, n_lev = sizes
    fields, levels, cells = x.shape
    stencil = dep.shape[0]
    blocks, slots = sp.shape
    rows = fields * levels
    groups = cells // LOW
    share = cells // n_lev
    per_lev = share // LOW
    panel, tile, lev = (lax.axis_index(a) for a in ("panel", "tile", "lev"))
    shift_cell = cells.bit_length() - 1
    shift_low = LOW.bit_length() - 1

    loads = [
        pltpu.make_async_copy(src, dst, in_sem.at[i])
        for i, (src, dst) in enumerate(((w_hbm, w.at[0]), (sp_hbm, sp), (dep_hbm, dep), (x_hbm, x)))
    ]
    for load in loads:
        load.start()

    barrier = pltpu.get_barrier_semaphore()

    def greet(device):
        pl.semaphore_signal(barrier, inc=1, device_id=device, device_id_type=MESH)

    has_prev, has_next = tile > 0, tile < n_tile - 1
    next_panel, prev_panel = lax.rem(panel + 1, n_panel), lax.rem(panel + n_panel - 1, n_panel)
    for d in range(1, n_lev):
        greet({"lev": lax.rem(lev + d, n_lev)})
    greet({"panel": prev_panel})
    greet({"panel": next_panel})

    @pl.when(has_prev)
    def _():
        greet({"tile": tile - 1})

    @pl.when(has_next)
    def _():
        greet({"tile": tile + 1})

    loads[0].wait()
    pl.semaphore_wait(barrier, n_lev + 1 + has_prev.astype(I32) + has_next.astype(I32))

    w_copies = [
        pltpu.make_async_remote_copy(
            src_ref=w.at[0],
            dst_ref=w.at[n_lev - d],
            send_sem=w_send.at[d - 1],
            recv_sem=w_recv.at[n_lev - d - 1],
            device_id={"lev": lax.rem(lev + d, n_lev)},
            device_id_type=MESH,
        )
        for d in range(1, n_lev)
    ]
    for copy in w_copies:
        copy.start()

    loads[1].wait()
    loads[2].wait()
    loads[3].wait()

    point = [sp[j : j + 1, :] for j in range(blocks)]
    cell_high = [(p & (cells - 1)) >> shift_low for p in point]
    stencil_of = [p >> shift_cell for p in point]
    lane = lax.broadcasted_iota(I32, (1, slots), 1)
    live = [lane < count_ref[j] for j in range(blocks)]
    for j in range(blocks):
        hot[:, j * slots : (j + 1) * slots] = one_hot(point[j] & (LOW - 1), slots)

    number = lax.broadcasted_iota(I32, (stencil * groups, slots), 0)
    marks = [
        jnp.where((number == (point[j] >> shift_low)) & live[j], 1.0, 0.0).astype(BF16)
        for j in range(blocks)
    ]
    sent[...] = times_transposed(jnp.concatenate(marks, axis=1), hot[...])

    height = 2 * rows + 16
    for g in range(groups):
        part = x[:, :, g * LOW : (g + 1) * LOW].reshape(rows, LOW)
        d4 = dep[:, g * LOW : (g + 1) * LOW]
        d8 = jnp.concatenate([d4 >> shift_low, d4 & (LOW - 1)], axis=0).astype(F32)
        d16 = jnp.concatenate([d8, jnp.zeros((8, LOW), F32)], axis=0).astype(BF16)
        glhs[g * height : g * height + 2 * rows, :] = split_rows(part)
        glhs[g * height + 2 * rows : (g + 1) * height, :] = d16
    row8 = lax.broadcasted_iota(I32, (8, slots), 0)
    for n in range(blocks * slots // LOW):
        found = jnp.dot(glhs[...], hot[:, n * LOW : (n + 1) * LOW], preferred_element_type=F32)
        for i in range(LOW // slots):
            j = n * (LOW // slots) + i
            total = jnp.zeros((height, slots), F32)
            for g in range(groups):
                piece = found[g * height : (g + 1) * height, i * slots : (i + 1) * slots]
                total = total + jnp.where(cell_high[j] == g, piece, 0.0)
            picked[j] = total[:rows] + total[rows : 2 * rows]
            scale = jnp.where(row8 < stencil, float(LOW), 1.0)
            own = (row8 & (stencil - 1)) == stencil_of[j]
            target = jnp.sum(
                jnp.where(own, total[2 * rows : 2 * rows + 8] * scale, 0.0), axis=0, keepdims=True
            )
            pay[j, rows : rows + 8, :] = jnp.broadcast_to(target, (8, slots))

    def segment(d):
        first = lax.rem(lev + d, n_lev)
        result = None
        for i in range(per_lev):
            at = pl.ds(pl.multiple_of(first * share + i * LOW, LOW), LOW)
            part = x[:, :, at].reshape(rows, LOW)
            for k in range(stencil):
                weight = w[d, k : k + 1, i * LOW : (i + 1) * LOW]
                landing = dep[k : k + 1, at]
                gone = sent[pl.ds(k * groups + first * per_lev + i, 1), :]
                high = jnp.where(gone > 0.5, groups, landing >> shift_low)
                term = spread(part * weight, high, landing & (LOW - 1), groups)
                result = term if result is None else result + term
        return result

    acc[...] = segment(0)

    for copy in w_copies:
        copy.wait_recv()

    wlhs = []
    for d in range(n_lev):
        for i in range(per_lev):
            w4 = w[d, :, i * LOW : (i + 1) * LOW]
            b1 = w4.astype(BF16).astype(F32)
            b2 = (w4 - b1).astype(BF16).astype(F32)
            wlhs.append(
                jnp.concatenate([b1, b2, w4 - b1 - b2, jnp.zeros_like(w4)], axis=0).astype(BF16)
            )
    found = jnp.dot(jnp.concatenate(wlhs, axis=0), hot[...], preferred_element_type=F32)
    row16 = lax.broadcasted_iota(I32, (16, slots), 0)
    for j in range(blocks):
        total = jnp.zeros((16, slots), F32)
        for d in range(n_lev):
            for i in range(per_lev):
                r = d * per_lev + i
                g = lax.rem(lev + d, n_lev) * per_lev + i
                piece = found[r * 16 : (r + 1) * 16, j * slots : (j + 1) * slots]
                total = total + jnp.where(cell_high[j] == g, piece, 0.0)
        own = (row16 & (stencil - 1)) == stencil_of[j]
        weight = jnp.sum(jnp.where(own, total, 0.0), axis=0, keepdims=True)
        weight = jnp.where(live[j], weight, 0.0)
        value = picked[j] * weight
        if j >= 2:
            code = turn_ref[j - 2]
            cosine = jnp.where(code == 0, 1.0, 0.0) - jnp.where(code == 2, 1.0, 0.0)
            sine = jnp.where(code == 1, 1.0, 0.0) - jnp.where(code == 3, 1.0, 0.0)
            zonal, merid = value[:levels], value[levels : 2 * levels]
            value = jnp.concatenate(
                [cosine * zonal + sine * merid, cosine * merid - sine * zonal, value[2 * levels :]],
                axis=0,
            )
        pay[j, 0:rows, :] = value

    def block_copy(j, device):
        return pltpu.make_async_remote_copy(
            src_ref=pay.at[j],
            dst_ref=recv.at[j],
            send_sem=p_send.at[j],
            recv_sem=p_recv.at[j],
            device_id=device,
            device_id_type=MESH,
        )

    copies = [
        block_copy(0, {"tile": jnp.maximum(tile - 1, 0)}),
        block_copy(1, {"tile": jnp.minimum(tile + 1, n_tile - 1)}),
        block_copy(2, {"panel": prev_panel}),
        block_copy(3, {"panel": next_panel}),
    ]

    @pl.when(has_prev)
    def _():
        copies[0].start()

    @pl.when(has_next)
    def _():
        copies[1].start()

    copies[2].start()
    copies[3].start()

    for d in (1, 3, 2):
        acc[...] += segment(d)

    for j, (there, here) in enumerate(((has_prev, has_next), (has_next, has_prev))):

        @pl.when(here)
        def _():
            copies[j].wait_recv()

        @pl.when(jnp.logical_not(here))
        def _():
            recv[j] = jnp.zeros_like(recv[j])

    copies[2].wait_recv()
    copies[3].wait_recv()

    result = acc[...]
    for n in range(blocks * slots // LOW):
        pair = [recv[n * (LOW // slots) + i] for i in range(LOW // slots)]
        value = jnp.concatenate([p[:rows] for p in pair], axis=1)
        landing = jnp.concatenate([p[rows : rows + 1] for p in pair], axis=1).astype(I32)
        result = result + spread(value, landing >> shift_low, landing & (LOW - 1), groups)
    for g in range(groups):
        top = g * 2 * rows
        out_ref[:, :, g * LOW : (g + 1) * LOW] = (
            result[top : top + rows] + result[top + rows : top + 2 * rows]
        ).reshape(fields, levels, LOW)

    for copy in w_copies:
        copy.wait_send()
    for j, there in enumerate((has_prev, has_next)):

        @pl.when(there)
        def _():
            copies[j].wait_send()

    copies[2].wait_send()
    copies[3].wait_send()


def body(sizes, adjoint_new, weights, departure, send_point, block_count, rotation):
    fields, levels, cells = adjoint_new.shape
    stencil = departure.shape[0]
    blocks, slots = send_point.shape
    rows = fields * levels
    groups = cells // LOW
    n_lev = sizes[2]
    hbm = pl.BlockSpec(memory_space=pl.ANY)
    smem = pl.BlockSpec(memory_space=pltpu.SMEM)
    return pl.pallas_call(
        functools.partial(kernel, sizes),
        out_shape=jax.ShapeDtypeStruct(adjoint_new.shape, F32),
        in_specs=[hbm, hbm, hbm, hbm, smem, smem],
        out_specs=pl.BlockSpec(memory_space=pltpu.VMEM),
        scratch_shapes=[
            pltpu.VMEM((fields, levels, cells), F32),
            pltpu.VMEM((n_lev, stencil, cells // n_lev), F32),
            pltpu.VMEM((stencil, cells), I32),
            pltpu.VMEM((blocks, slots), I32),
            pltpu.VMEM((LOW, blocks * slots), BF16),
            pltpu.VMEM((groups * (2 * rows + 16), LOW), BF16),
            pltpu.VMEM((stencil * groups, LOW), F32),
            pltpu.VMEM((blocks, rows, slots), F32),
            pltpu.VMEM((groups * 2 * rows, LOW), F32),
            pltpu.VMEM((blocks, rows + 8, slots), F32),
            pltpu.VMEM((blocks, rows + 8, slots), F32),
            pltpu.SemaphoreType.DMA((4,)),
            pltpu.SemaphoreType.DMA((n_lev - 1,)),
            pltpu.SemaphoreType.DMA((n_lev - 1,)),
            pltpu.SemaphoreType.DMA((blocks,)),
            pltpu.SemaphoreType.DMA((blocks,)),
        ],
        compiler_params=pltpu.CompilerParams(collective_id=0, has_side_effects=True),
    )(adjoint_new, weights, departure, send_point, block_count.reshape(-1), rotation.reshape(-1))


def solution(mesh):
    sizes = tuple(mesh.shape[a] for a in ("panel", "tile", "lev"))
    return jax.shard_map(
        functools.partial(body, sizes),
        mesh=mesh,
        in_specs=(
            P(None, "lev", ("panel", "tile")),
            P(None, ("panel", "tile", "lev")),
            P(None, ("panel", "tile")),
            P(None, ("panel", "tile")),
            P(None, ("panel", "tile")),
            P(None, ("panel", "tile")),
        ),
        out_specs=P(None, "lev", ("panel", "tile")),
        check_vma=False,
    )
```

```python
import functools

import jax
import jax.numpy as jnp
from jax import lax
from jax.experimental import pallas as pl
from jax.experimental.pallas import tpu as pltpu
from jax.sharding import PartitionSpec as P

MESH = pl.DeviceIdType.MESH
LOW = 256
F32, BF16, I32 = jnp.float32, jnp.bfloat16, jnp.int32


def split_rows(value):
    high = value.astype(BF16).astype(F32)
    return jnp.concatenate([high, value - high], axis=0).astype(BF16)


def one_hot(low, columns):
    rows = lax.broadcasted_iota(I32, (LOW, columns), 0)
    return jnp.where(rows == low, 1.0, 0.0).astype(BF16)


def times_transposed(lhs, rhs):
    return lax.dot_general(lhs, rhs, (((1,), (1,)), ((), ())), preferred_element_type=F32)


def spread(value, target_high, target_low, groups):
    parts = split_rows(value)
    copies = parts.shape[0] // 16
    high = jnp.broadcast_to(target_high, (16, LOW))
    lhs = []
    for g in range(groups):
        mask = jnp.where(high == g, 1.0, 0.0).astype(BF16)
        lhs.append(parts * jnp.concatenate([mask] * copies, axis=0))
    return times_transposed(jnp.concatenate(lhs, axis=0), one_hot(target_low, LOW))


def kernel(
    sizes,
    x_hbm,
    w_hbm,
    dep_hbm,
    sp_hbm,
    count_hbm,
    turn_hbm,
    out_ref,
    count_ref,
    turn_ref,
    x,
    w,
    dep,
    sp,
    hot,
    glhs,
    sent,
    picked,
    acc,
    pay,
    recv,
    in_sem,
    w_send,
    w_recv,
    p_send,
    p_recv,
):
    n_panel, n_tile, n_lev = sizes
    fields, levels, cells = x.shape
    stencil = dep.shape[0]
    blocks, slots = sp.shape
    rows = fields * levels
    groups = cells // LOW
    share = cells // n_lev
    per_lev = share // LOW
    panel, tile, lev = (lax.axis_index(a) for a in ("panel", "tile", "lev"))
    shift_cell = cells.bit_length() - 1
    shift_low = LOW.bit_length() - 1

    loads = [
        pltpu.make_async_copy(src, dst, in_sem.at[i])
        for i, (src, dst) in enumerate(
            (
                (w_hbm, w.at[0]),
                (sp_hbm, sp),
                (dep_hbm, dep),
                (x_hbm, x),
                (count_hbm, count_ref),
                (turn_hbm, turn_ref),
            )
        )
    ]
    for load in loads:
        load.start()

    barrier = pltpu.get_barrier_semaphore()

    def greet(device):
        pl.semaphore_signal(barrier, inc=1, device_id=device, device_id_type=MESH)

    has_prev, has_next = tile > 0, tile < n_tile - 1
    next_panel, prev_panel = lax.rem(panel + 1, n_panel), lax.rem(panel + n_panel - 1, n_panel)
    for d in range(1, n_lev):
        greet({"lev": lax.rem(lev + d, n_lev)})
    greet({"panel": prev_panel})
    greet({"panel": next_panel})

    @pl.when(has_prev)
    def _():
        greet({"tile": tile - 1})

    @pl.when(has_next)
    def _():
        greet({"tile": tile + 1})

    for load in loads[1:]:
        load.wait()

    point = [sp[j : j + 1, :] for j in range(blocks)]
    cell_high = [(p & (cells - 1)) >> shift_low for p in point]
    stencil_of = [p >> shift_cell for p in point]
    lane = lax.broadcasted_iota(I32, (1, slots), 1)
    live = [lane < count_ref[j] for j in range(blocks)]
    for j in range(blocks):
        hot[:, j * slots : (j + 1) * slots] = one_hot(point[j] & (LOW - 1), slots)

    number = lax.broadcasted_iota(I32, (stencil * groups, slots), 0)
    marks = [
        jnp.where((number == (point[j] >> shift_low)) & live[j], 1.0, 0.0).astype(BF16)
        for j in range(blocks)
    ]
    sent[...] = times_transposed(jnp.concatenate(marks, axis=1), hot[...])

    height = 2 * rows + 16
    for g in range(groups):
        part = x[:, :, g * LOW : (g + 1) * LOW].reshape(rows, LOW)
        d4 = dep[:, g * LOW : (g + 1) * LOW]
        d8 = jnp.concatenate([d4 >> shift_low, d4 & (LOW - 1)], axis=0).astype(F32)
        d16 = jnp.concatenate([d8, jnp.zeros((8, LOW), F32)], axis=0).astype(BF16)
        glhs[g * height : g * height + 2 * rows, :] = split_rows(part)
        glhs[g * height + 2 * rows : (g + 1) * height, :] = d16
    row8 = lax.broadcasted_iota(I32, (8, slots), 0)
    for n in range(blocks * slots // LOW):
        found = jnp.dot(glhs[...], hot[:, n * LOW : (n + 1) * LOW], preferred_element_type=F32)
        for i in range(LOW // slots):
            j = n * (LOW // slots) + i
            total = jnp.zeros((height, slots), F32)
            for g in range(groups):
                piece = found[g * height : (g + 1) * height, i * slots : (i + 1) * slots]
                total = total + jnp.where(cell_high[j] == g, piece, 0.0)
            picked[j] = total[:rows] + total[rows : 2 * rows]
            scale = jnp.where(row8 < stencil, float(LOW), 1.0)
            own = (row8 & (stencil - 1)) == stencil_of[j]
            target = jnp.sum(
                jnp.where(own, total[2 * rows : 2 * rows + 8] * scale, 0.0), axis=0, keepdims=True
            )
            pay[j, rows : rows + 8, :] = jnp.broadcast_to(target, (8, slots))

    loads[0].wait()
    pl.semaphore_wait(barrier, n_lev + 1 + has_prev.astype(I32) + has_next.astype(I32))

    w_copies = [
        pltpu.make_async_remote_copy(
            src_ref=w.at[0],
            dst_ref=w.at[n_lev - d],
            send_sem=w_send.at[d - 1],
            recv_sem=w_recv.at[n_lev - d - 1],
            device_id={"lev": lax.rem(lev + d, n_lev)},
            device_id_type=MESH,
        )
        for d in range(1, n_lev)
    ]
    for copy in w_copies:
        copy.start()

    def segment(d):
        first = lax.rem(lev + d, n_lev)
        result = None
        for i in range(per_lev):
            at = pl.ds(pl.multiple_of(first * share + i * LOW, LOW), LOW)
            part = x[:, :, at].reshape(rows, LOW)
            for k in range(stencil):
                weight = w[d, k : k + 1, i * LOW : (i + 1) * LOW]
                landing = dep[k : k + 1, at]
                gone = sent[pl.ds(k * groups + first * per_lev + i, 1), :]
                high = jnp.where(gone > 0.5, groups, landing >> shift_low)
                term = spread(part * weight, high, landing & (LOW - 1), groups)
                result = term if result is None else result + term
        return result

    acc[...] = segment(0)

    for copy in w_copies:
        copy.wait_recv()

    wlhs = []
    for d in range(n_lev):
        for i in range(per_lev):
            w4 = w[d, :, i * LOW : (i + 1) * LOW]
            b1 = w4.astype(BF16).astype(F32)
            b2 = (w4 - b1).astype(BF16).astype(F32)
            wlhs.append(
                jnp.concatenate([b1, b2, w4 - b1 - b2, jnp.zeros_like(w4)], axis=0).astype(BF16)
            )
    found = jnp.dot(jnp.concatenate(wlhs, axis=0), hot[...], preferred_element_type=F32)
    row16 = lax.broadcasted_iota(I32, (16, slots), 0)
    for j in range(blocks):
        total = jnp.zeros((16, slots), F32)
        for d in range(n_lev):
            for i in range(per_lev):
                r = d * per_lev + i
                g = lax.rem(lev + d, n_lev) * per_lev + i
                piece = found[r * 16 : (r + 1) * 16, j * slots : (j + 1) * slots]
                total = total + jnp.where(cell_high[j] == g, piece, 0.0)
        own = (row16 & (stencil - 1)) == stencil_of[j]
        weight = jnp.sum(jnp.where(own, total, 0.0), axis=0, keepdims=True)
        weight = jnp.where(live[j], weight, 0.0)
        value = picked[j] * weight
        if j >= 2:
            code = turn_ref[j - 2]
            cosine = jnp.where(code == 0, 1.0, 0.0) - jnp.where(code == 2, 1.0, 0.0)
            sine = jnp.where(code == 1, 1.0, 0.0) - jnp.where(code == 3, 1.0, 0.0)
            zonal, merid = value[:levels], value[levels : 2 * levels]
            value = jnp.concatenate(
                [cosine * zonal + sine * merid, cosine * merid - sine * zonal, value[2 * levels :]],
                axis=0,
            )
        pay[j, 0:rows, :] = value

    def block_copy(j, device):
        return pltpu.make_async_remote_copy(
            src_ref=pay.at[j],
            dst_ref=recv.at[j],
            send_sem=p_send.at[j],
            recv_sem=p_recv.at[j],
            device_id=device,
            device_id_type=MESH,
        )

    copies = [
        block_copy(0, {"tile": jnp.maximum(tile - 1, 0)}),
        block_copy(1, {"tile": jnp.minimum(tile + 1, n_tile - 1)}),
        block_copy(2, {"panel": prev_panel}),
        block_copy(3, {"panel": next_panel}),
    ]

    @pl.when(has_prev)
    def _():
        copies[0].start()

    @pl.when(has_next)
    def _():
        copies[1].start()

    copies[2].start()
    copies[3].start()

    for d in (1, 3, 2):
        acc[...] += segment(d)

    for j, (there, here) in enumerate(((has_prev, has_next), (has_next, has_prev))):

        @pl.when(here)
        def _():
            copies[j].wait_recv()

        @pl.when(jnp.logical_not(here))
        def _():
            recv[j] = jnp.zeros_like(recv[j])

    copies[2].wait_recv()
    copies[3].wait_recv()

    result = acc[...]
    for n in range(blocks * slots // LOW):
        pair = [recv[n * (LOW // slots) + i] for i in range(LOW // slots)]
        value = jnp.concatenate([p[:rows] for p in pair], axis=1)
        landing = jnp.concatenate([p[rows : rows + 1] for p in pair], axis=1).astype(I32)
        result = result + spread(value, landing >> shift_low, landing & (LOW - 1), groups)
    for g in range(groups):
        top = g * 2 * rows
        out_ref[:, :, g * LOW : (g + 1) * LOW] = (
            result[top : top + rows] + result[top + rows : top + 2 * rows]
        ).reshape(fields, levels, LOW)

    for copy in w_copies:
        copy.wait_send()
    for j, there in enumerate((has_prev, has_next)):

        @pl.when(there)
        def _():
            copies[j].wait_send()

    copies[2].wait_send()
    copies[3].wait_send()


def body(sizes, adjoint_new, weights, departure, send_point, block_count, rotation):
    fields, levels, cells = adjoint_new.shape
    stencil = departure.shape[0]
    blocks, slots = send_point.shape
    rows = fields * levels
    groups = cells // LOW
    n_lev = sizes[2]
    hbm = pl.BlockSpec(memory_space=pltpu.HBM)
    args = (adjoint_new, weights, departure, send_point, block_count.reshape(-1), rotation.reshape(-1))
    return pl.pallas_call(
        functools.partial(kernel, sizes),
        out_shape=pltpu.VMEM(adjoint_new.shape, F32),
        in_specs=[hbm] * len(args),
        out_specs=pl.BlockSpec(memory_space=pltpu.VMEM),
        scratch_shapes=[
            pltpu.SMEM((blocks,), I32),
            pltpu.SMEM((rotation.shape[0],), I32),
            pltpu.VMEM((fields, levels, cells), F32),
            pltpu.VMEM((n_lev, stencil, cells // n_lev), F32),
            pltpu.VMEM((stencil, cells), I32),
            pltpu.VMEM((blocks, slots), I32),
            pltpu.VMEM((LOW, blocks * slots), BF16),
            pltpu.VMEM((groups * (2 * rows + 16), LOW), BF16),
            pltpu.VMEM((stencil * groups, LOW), F32),
            pltpu.VMEM((blocks, rows, slots), F32),
            pltpu.VMEM((groups * 2 * rows, LOW), F32),
            pltpu.VMEM((blocks, rows + 8, slots), F32),
            pltpu.VMEM((blocks, rows + 8, slots), F32),
            pltpu.SemaphoreType.DMA((len(args),)),
            pltpu.SemaphoreType.DMA((n_lev - 1,)),
            pltpu.SemaphoreType.DMA((n_lev - 1,)),
            pltpu.SemaphoreType.DMA((blocks,)),
            pltpu.SemaphoreType.DMA((blocks,)),
        ],
        compiler_params=pltpu.CompilerParams(
            collective_id=0, has_side_effects=True, vmem_limit_bytes=16 * 1024 * 1024
        ),
    )(*(pltpu.with_memory_space_constraint(a, pltpu.HBM) for a in args))


def solution(mesh):
    sizes = tuple(mesh.shape[a] for a in ("panel", "tile", "lev"))
    return jax.shard_map(
        functools.partial(body, sizes),
        mesh=mesh,
        in_specs=(
            P(None, "lev", ("panel", "tile")),
            P(None, ("panel", "tile", "lev")),
            P(None, ("panel", "tile")),
            P(None, ("panel", "tile")),
            P(None, ("panel", "tile")),
            P(None, ("panel", "tile")),
        ),
        out_specs=P(None, "lev", ("panel", "tile")),
        check_vma=False,
    )
```

```python
import functools

import jax
import jax.numpy as jnp
from jax import lax
from jax.experimental import pallas as pl
from jax.experimental.pallas import tpu as pltpu
from jax.sharding import PartitionSpec as P

MESH = pl.DeviceIdType.MESH
LOW = 256
F32, BF16, I32 = jnp.float32, jnp.bfloat16, jnp.int32


def split_rows(value):
    high = value.astype(BF16).astype(F32)
    return jnp.concatenate([high, value - high], axis=0).astype(BF16)


def one_hot(low, columns):
    rows = lax.broadcasted_iota(I32, (LOW, columns), 0)
    return jnp.where(rows == low, 1.0, 0.0).astype(BF16)


def times_transposed(lhs, rhs):
    return lax.dot_general(lhs, rhs, (((1,), (1,)), ((), ())), preferred_element_type=F32)


def spread(value, target_high, target_low, groups):
    parts = split_rows(value)
    copies = parts.shape[0] // 16
    high = jnp.broadcast_to(target_high, (16, LOW))
    lhs = []
    for g in range(groups):
        mask = jnp.where(high == g, 1.0, 0.0).astype(BF16)
        lhs.append(parts * jnp.concatenate([mask] * copies, axis=0))
    return times_transposed(jnp.concatenate(lhs, axis=0), one_hot(target_low, LOW))


def kernel(
    sizes,
    x_hbm,
    w_hbm,
    dep_hbm,
    sp_hbm,
    count_hbm,
    turn_hbm,
    out_ref,
    count_ref,
    turn_ref,
    x,
    w,
    relay,
    dep,
    sp,
    hot,
    glhs,
    sent,
    acc,
    pay,
    recv,
    extra,
    in_sem,
    w_send,
    w_recv,
    r_recv,
    z_send,
    z_recv,
    p_send,
    p_recv,
    e_send,
    e_recv,
):
    n_panel, n_tile, n_lev = sizes
    fields, levels, cells = x.shape
    stencil = dep.shape[0]
    blocks, slots = sp.shape
    rows = fields * levels
    groups = cells // LOW
    share = cells // n_lev
    per_lev = share // LOW
    panel, tile, lev = (lax.axis_index(a) for a in ("panel", "tile", "lev"))
    shift_cell = cells.bit_length() - 1
    shift_low = LOW.bit_length() - 1
    at_slot = rows + 8

    odd = lax.rem(tile, 2) == 1
    even = jnp.logical_not(odd)
    first = lev == 0
    lone = jnp.logical_and(even, first)
    helper = jnp.logical_and(odd, first)
    feeder = jnp.logical_and(even, jnp.logical_not(first))
    second = jnp.logical_and(even, lev == 1)
    other = jnp.logical_and(odd, jnp.logical_not(first))
    has_prev, has_next = tile > 0, tile < n_tile - 1
    yes = tile >= 0
    next_panel, prev_panel = lax.rem(panel + 1, n_panel), lax.rem(panel + n_panel - 1, n_panel)
    prev_tile, next_tile = jnp.maximum(tile - 1, 0), jnp.minimum(tile + 1, n_tile - 1)
    toward = [{"tile": prev_tile}, {"tile": next_tile}, {"panel": prev_panel}, {"panel": next_panel}]
    sends_to = [has_prev, has_next, yes, yes]
    comes_from = [{"tile": next_tile}, {"tile": prev_tile}, {"panel": next_panel}, {"panel": prev_panel}]
    hears = [has_next, has_prev, yes, yes]
    from_even = [odd, odd, even, even]

    loads = [
        pltpu.make_async_copy(src, dst, in_sem.at[i])
        for i, (src, dst) in enumerate(
            (
                (sp_hbm, sp),
                (w_hbm, w.at[lev]),
                (count_hbm, count_ref),
                (turn_hbm, turn_ref),
                (dep_hbm, dep),
                (x_hbm, x),
            )
        )
    ]
    for load in loads:
        load.start()

    barrier = pltpu.get_barrier_semaphore()

    def greet(device):
        pl.semaphore_signal(barrier, inc=1, device_id=device, device_id_type=MESH)

    @pl.when(lone)
    def _():
        greet({"tile": next_tile})

    @pl.when(jnp.logical_not(lone))
    def _():
        for d in range(1, n_lev):
            greet({"lev": lax.rem(lev + d, n_lev)})
        for j in range(blocks):

            @pl.when(hears[j])
            def _(j=j):
                greet(comes_from[j])

                @pl.when(from_even[j])
                def _():
                    greet({**comes_from[j], "lev": jnp.where(first, 1, 0)})

    @pl.when(helper)
    def _():
        for t in range(1, n_lev):
            greet({"tile": prev_tile, "lev": t})
        for p in (prev_panel, next_panel):
            for t in range(2):
                greet({"panel": p, "tile": prev_tile, "lev": t})

        @pl.when(tile > 1)
        def _():
            greet({"tile": tile - 2})

    acc[...] = jnp.zeros_like(acc)

    sent_blocks = 2 + has_prev.astype(I32) + has_next.astype(I32)
    more = jnp.where(lone, n_lev - 1, 0) + jnp.where(second, 1, 0)

    def weight_copy(d, dst, sem, device):
        return pltpu.make_async_remote_copy(
            src_ref=w.at[lev],
            dst_ref=dst.at[lev],
            send_sem=w_send.at[d - 1],
            recv_sem=sem.at[lev],
            device_id=device,
            device_id_type=MESH,
        )

    def enter():
        pl.semaphore_wait(barrier, n_lev - 1 + sent_blocks * (1 + more))
        for d in range(1, n_lev):
            indirect = jnp.logical_and(even, lev == n_lev - d)

            @pl.when(indirect)
            def _(d=d):
                weight_copy(d, relay, r_recv, {"tile": next_tile, "lev": 0}).start()

            @pl.when(jnp.logical_not(indirect))
            def _(d=d):
                weight_copy(d, w, w_recv, {"lev": lax.rem(lev + d, n_lev)}).start()

    for load in loads[:2]:
        load.wait()

    @pl.when(lone)
    def _():
        enter()

    for load in loads[2:4]:
        load.wait()

    point = [sp[j : j + 1, :] for j in range(blocks)]
    cell_high = [(p & (cells - 1)) >> shift_low for p in point]
    stencil_of = [p >> shift_cell for p in point]
    lane = lax.broadcasted_iota(I32, (1, slots), 1)
    live = [lane < count_ref[j] for j in range(blocks)]
    for j in range(blocks):
        hot[:, j * slots : (j + 1) * slots] = one_hot(point[j] & (LOW - 1), slots)

    def slot_weights(parts):
        lhs = []
        for t in parts:
            for i in range(per_lev):
                w4 = w[t, :, i * LOW : (i + 1) * LOW]
                b1 = w4.astype(BF16).astype(F32)
                b2 = (w4 - b1).astype(BF16).astype(F32)
                lhs.append(
                    jnp.concatenate([b1, b2, w4 - b1 - b2, jnp.zeros_like(w4)], axis=0).astype(BF16)
                )
        found = jnp.dot(jnp.concatenate(lhs, axis=0), hot[...], preferred_element_type=F32)
        row16 = lax.broadcasted_iota(I32, (16, slots), 0)
        result = []
        for j in range(blocks):
            total = jnp.zeros((16, slots), F32)
            for n, t in enumerate(parts):
                for i in range(per_lev):
                    r = n * per_lev + i
                    piece = found[r * 16 : (r + 1) * 16, j * slots : (j + 1) * slots]
                    total = total + jnp.where(cell_high[j] == t * per_lev + i, piece, 0.0)
            own = (row16 & (stencil - 1)) == stencil_of[j]
            weight = jnp.sum(jnp.where(own, total, 0.0), axis=0, keepdims=True)
            result.append(jnp.where(live[j], weight, 0.0))
        return result

    for j, weight in enumerate(slot_weights([lev])):
        pay[j, at_slot:, :] = jnp.broadcast_to(weight, (8, slots))

    def ahead(j, moved):
        if j >= 2:
            return {**toward[j], "tile": tile + moved}
        return {"tile": toward[j]["tile"] + moved}

    def block_copy(j):
        moved = jnp.where(helper, 1, 0) if j == 1 else (jnp.where(lone, 1, 0) if j >= 2 else 0)
        return pltpu.make_async_remote_copy(
            src_ref=pay.at[j],
            dst_ref=recv.at[j + blocks * moved],
            send_sem=p_send.at[j],
            recv_sem=p_recv.at[j + blocks * moved],
            device_id=ahead(j, moved),
            device_id_type=MESH,
        )

    def extra_copy(j, n, level):
        moved = jnp.where(second, 1, 0) if level == 0 and j >= 2 else 0
        return pltpu.make_async_remote_copy(
            src_ref=pay.at[j, pl.ds(at_slot, 8)],
            dst_ref=extra.at[j + blocks * moved],
            send_sem=e_send.at[j, n],
            recv_sem=e_recv.at[j + blocks * moved],
            device_id={**ahead(j, moved), "lev": level},
            device_id_type=MESH,
        )

    def send_blocks():
        for j in (1, 0, 2, 3):

            @pl.when(sends_to[j])
            def _(j=j):
                block_copy(j).start()

    @pl.when(lone)
    def _():
        for t in range(1, n_lev):
            for j in (1, 0, 2, 3):

                @pl.when(sends_to[j])
                def _(j=j, t=t):
                    extra_copy(j, t - 1, t).start()

    for load in loads[4:]:
        load.wait()

    height = 2 * rows + 16
    for g in range(groups):
        part = x[:, :, g * LOW : (g + 1) * LOW].reshape(rows, LOW)
        d4 = dep[:, g * LOW : (g + 1) * LOW]
        d8 = jnp.concatenate([d4 >> shift_low, d4 & (LOW - 1)], axis=0).astype(F32)
        d16 = jnp.concatenate([d8, jnp.zeros((8, LOW), F32)], axis=0).astype(BF16)
        glhs[g * height : g * height + 2 * rows, :] = split_rows(part)
        glhs[g * height + 2 * rows : (g + 1) * height, :] = d16
    row8 = lax.broadcasted_iota(I32, (8, slots), 0)
    for n in range(blocks * slots // LOW):
        found = jnp.dot(glhs[...], hot[:, n * LOW : (n + 1) * LOW], preferred_element_type=F32)
        for i in range(LOW // slots):
            j = n * (LOW // slots) + i
            total = jnp.zeros((height, slots), F32)
            for g in range(groups):
                piece = found[g * height : (g + 1) * height, i * slots : (i + 1) * slots]
                total = total + jnp.where(cell_high[j] == g, piece, 0.0)
            value = total[:rows] + total[rows : 2 * rows]
            if j >= 2:
                code = turn_ref[j - 2]
                cosine = jnp.where(code == 0, 1.0, 0.0) - jnp.where(code == 2, 1.0, 0.0)
                sine = jnp.where(code == 1, 1.0, 0.0) - jnp.where(code == 3, 1.0, 0.0)
                zonal, merid = value[:levels], value[levels : 2 * levels]
                value = jnp.concatenate(
                    [
                        cosine * zonal + sine * merid,
                        cosine * merid - sine * zonal,
                        value[2 * levels :],
                    ],
                    axis=0,
                )
            scale = jnp.where(row8 < stencil, float(LOW), 1.0)
            own = (row8 & (stencil - 1)) == stencil_of[j]
            target = jnp.sum(
                jnp.where(own, total[2 * rows : 2 * rows + 8] * scale, 0.0), axis=0, keepdims=True
            )
            pay[j, 0:rows, :] = value
            pay[j, rows:at_slot, :] = jnp.broadcast_to(target, (8, slots))

    @pl.when(lone)
    def _():
        send_blocks()

    number = lax.broadcasted_iota(I32, (stencil * groups, slots), 0)
    marks = [
        jnp.where((number == (point[j] >> shift_low)) & live[j], 1.0, 0.0).astype(BF16)
        for j in range(blocks)
    ]
    sent[...] = times_transposed(jnp.concatenate(marks, axis=1), hot[...])

    def segment(t):
        result = None
        for i in range(per_lev):
            at = pl.ds(pl.multiple_of(t * share + i * LOW, LOW), LOW)
            part = x[:, :, at].reshape(rows, LOW)
            for k in range(stencil):
                weight = w[t, k : k + 1, i * LOW : (i + 1) * LOW]
                landing = dep[k : k + 1, at]
                gone = sent[pl.ds(k * groups + t * per_lev + i, 1), :]
                high = jnp.where(gone > 0.5, groups, landing >> shift_low)
                term = spread(part * weight, high, landing & (LOW - 1), groups)
                result = term if result is None else result + term
        return result

    order = [
        lev,
        jnp.where(first, 1, 1 + lax.rem(lev, 3)),
        jnp.where(first, 2, 1 + lax.rem(lev + 1, 3)),
        jnp.where(first, 3, 0),
    ]

    def arrival(buffer, sem, t):
        return pltpu.make_async_remote_copy(
            src_ref=buffer.at[t],
            dst_ref=buffer.at[t],
            send_sem=w_send.at[0],
            recv_sem=sem.at[t],
            device_id={"panel": next_panel},
            device_id_type=MESH,
        )

    def add_weights(parts):
        weights = slot_weights(parts)
        for j in range(blocks):
            pay[j, at_slot:, :] += jnp.broadcast_to(weights[j], (8, slots))
        send_blocks()

    def to_lone(src, dst, send_sem, recv_sem):
        return pltpu.make_async_remote_copy(
            src_ref=src,
            dst_ref=dst,
            send_sem=send_sem,
            recv_sem=recv_sem,
            device_id={"tile": prev_tile},
            device_id_type=MESH,
        )

    others = pl.ds(1, n_lev - 1)
    relay_copy = to_lone(relay.at[others], w.at[others], z_send.at[0], z_recv)
    passed_on = [
        (j, to_lone(recv.at[blocks + j], recv.at[j], z_send.at[j], p_recv.at[j]))
        for j in range(1, blocks)
    ]
    passed_on_extra = [
        (j, to_lone(extra.at[blocks + j], extra.at[j], z_send.at[j + 2], e_recv.at[j]))
        for j in (2, 3)
    ]

    def both(*conditions):
        return functools.reduce(jnp.logical_and, conditions)

    def step(i, carry):
        @pl.when(i == jnp.where(helper, 2, jnp.where(other, 1, jnp.where(feeder, 0, -1))))
        def _():
            enter()

        when = (
            jnp.where(lone, -1, 1),
            jnp.where(lone, -1, jnp.where(feeder, 1, 2)),
            jnp.where(lone, -1, jnp.where(helper, 2, jnp.where(other, 3, 4))),
        )
        for n in range(3):

            @pl.when(i == when[n])
            def _(n=n):
                arrival(w, w_recv, order[n + 1]).wait_recv()

        @pl.when(both(odd, i == when[2]))
        def _():
            add_weights(order[1:])

        @pl.when(both(feeder, i == 1))
        def _():
            add_weights(order[1:3])

            @pl.when(second)
            def _():
                for j in range(blocks):

                    @pl.when(sends_to[j])
                    def _(j=j):
                        extra_copy(j, 0, 0).start()

        @pl.when(both(helper, i == 2))
        def _():
            for t in range(1, n_lev):
                arrival(relay, r_recv, t).wait_recv()
            relay_copy.start()

        @pl.when(both(lone, i == 1))
        def _():
            relay_copy.wait_recv()

        @pl.when(both(helper, i == 4))
        def _():
            for j, copy in passed_on:

                @pl.when(tile > 1 if j == 1 else yes)
                def _(j=j, copy=copy):
                    arrival(recv, p_recv, blocks + j).wait_recv()
                    copy.start()

            for j, copy in passed_on_extra:
                arrival(extra, e_recv, blocks + j).wait_recv()
                copy.start()

        arriving = i == jnp.where(feeder, 3, 4)

        @pl.when(jnp.logical_not(arriving))
        def _():
            k = jnp.minimum(i, 3)
            t = jnp.where(
                k == 0, order[0], jnp.where(k == 1, order[1], jnp.where(k == 2, order[2], order[3]))
            )
            acc[...] += segment(t)

        @pl.when(arriving)
        def _():
            for j in range(blocks):

                @pl.when(hears[j])
                def _(j=j):
                    arrival(recv, p_recv, j).wait_recv()

                @pl.when(jnp.logical_not(hears[j]))
                def _(j=j):
                    recv[j] = jnp.zeros_like(recv[j])

                also = jnp.logical_and(hears[j], from_even[j])

                @pl.when(also)
                def _(j=j):
                    arrival(extra, e_recv, j).wait_recv()

                @pl.when(jnp.logical_not(also))
                def _(j=j):
                    extra[j] = jnp.zeros_like(extra[j])

            result = acc[...]
            for pair in ((0, 2), (1, 3)):
                value = jnp.concatenate(
                    [
                        recv[j, 0:rows] * (recv[j, at_slot : at_slot + 1] + extra[j, 0:1])
                        for j in pair
                    ],
                    axis=1,
                )
                landing = jnp.concatenate([recv[j, rows : rows + 1] for j in pair], axis=1).astype(I32)
                result = result + spread(value, landing >> shift_low, landing & (LOW - 1), groups)
            acc[...] = result

        return carry

    lax.fori_loop(0, 5, step, 0)

    result = acc
    for g in range(groups):
        top = g * 2 * rows
        out_ref[:, :, g * LOW : (g + 1) * LOW] = (
            result[top : top + rows, :] + result[top + rows : top + 2 * rows, :]
        ).reshape(fields, levels, LOW)

    for d in range(1, n_lev):
        weight_copy(d, w, w_recv, {"lev": lax.rem(lev + d, n_lev)}).wait_send()
    for j in range(blocks):

        @pl.when(sends_to[j])
        def _(j=j):
            block_copy(j).wait_send()

            @pl.when(lone)
            def _():
                for t in range(1, n_lev):
                    extra_copy(j, t - 1, t).wait_send()

            @pl.when(second)
            def _():
                extra_copy(j, 0, 0).wait_send()

    @pl.when(helper)
    def _():
        relay_copy.wait_send()
        for j, copy in passed_on:

            @pl.when(tile > 1 if j == 1 else yes)
            def _(copy=copy):
                copy.wait_send()

        for j, copy in passed_on_extra:
            copy.wait_send()


def body(sizes, adjoint_new, weights, departure, send_point, block_count, rotation):
    fields, levels, cells = adjoint_new.shape
    stencil = departure.shape[0]
    blocks, slots = send_point.shape
    rows = fields * levels
    groups = cells // LOW
    n_lev = sizes[2]
    hbm = pl.BlockSpec(memory_space=pltpu.HBM)
    args = (adjoint_new, weights, departure, send_point, block_count.reshape(-1), rotation.reshape(-1))
    return pl.pallas_call(
        functools.partial(kernel, sizes),
        out_shape=pltpu.VMEM(adjoint_new.shape, F32),
        in_specs=[hbm] * len(args),
        out_specs=pl.BlockSpec(memory_space=pltpu.VMEM),
        scratch_shapes=[
            pltpu.SMEM((blocks,), I32),
            pltpu.SMEM((rotation.shape[0],), I32),
            pltpu.VMEM((fields, levels, cells), F32),
            pltpu.VMEM((n_lev, stencil, cells // n_lev), F32),
            pltpu.VMEM((n_lev, stencil, cells // n_lev), F32),
            pltpu.VMEM((stencil, cells), I32),
            pltpu.VMEM((blocks, slots), I32),
            pltpu.VMEM((LOW, blocks * slots), BF16),
            pltpu.VMEM((groups * (2 * rows + 16), LOW), BF16),
            pltpu.VMEM((stencil * groups, LOW), F32),
            pltpu.VMEM((groups * 2 * rows, LOW), F32),
            pltpu.VMEM((blocks, rows + 16, slots), F32),
            pltpu.VMEM((2 * blocks, rows + 16, slots), F32),
            pltpu.VMEM((2 * blocks, 8, slots), F32),
            pltpu.SemaphoreType.DMA((len(args),)),
            pltpu.SemaphoreType.DMA((n_lev - 1,)),
            pltpu.SemaphoreType.DMA((n_lev,)),
            pltpu.SemaphoreType.DMA((n_lev,)),
            pltpu.SemaphoreType.DMA((blocks + 2,)),
            pltpu.SemaphoreType.DMA,
            pltpu.SemaphoreType.DMA((blocks,)),
            pltpu.SemaphoreType.DMA((2 * blocks,)),
            pltpu.SemaphoreType.DMA((blocks, n_lev - 1)),
            pltpu.SemaphoreType.DMA((2 * blocks,)),
        ],
        compiler_params=pltpu.CompilerParams(
            collective_id=0, has_side_effects=True, vmem_limit_bytes=16 * 1024 * 1024
        ),
    )(*(pltpu.with_memory_space_constraint(a, pltpu.HBM) for a in args))


def solution(mesh):
    sizes = tuple(mesh.shape[a] for a in ("panel", "tile", "lev"))
    return jax.shard_map(
        functools.partial(body, sizes),
        mesh=mesh,
        in_specs=(
            P(None, "lev", ("panel", "tile")),
            P(None, ("panel", "tile", "lev")),
            P(None, ("panel", "tile")),
            P(None, ("panel", "tile")),
            P(None, ("panel", "tile")),
            P(None, ("panel", "tile")),
        ),
        out_specs=P(None, "lev", ("panel", "tile")),
        check_vma=False,
    )
```

```python
import functools

import jax
import jax.numpy as jnp
from jax import lax
from jax.experimental import pallas as pl
from jax.experimental.pallas import tpu as pltpu
from jax.sharding import PartitionSpec as P

MESH = pl.DeviceIdType.MESH
LOW = 256
F32, BF16, I32 = jnp.float32, jnp.bfloat16, jnp.int32


def split_rows(value):
    high = value.astype(BF16).astype(F32)
    return jnp.concatenate([high, value - high], axis=0).astype(BF16)


def one_hot(low, columns):
    rows = lax.broadcasted_iota(I32, (LOW, columns), 0)
    return jnp.where(rows == low, 1.0, 0.0).astype(BF16)


def times_transposed(lhs, rhs):
    return lax.dot_general(lhs, rhs, (((1,), (1,)), ((), ())), preferred_element_type=F32)


def spread(value, target_high, target_low, groups):
    parts = split_rows(value)
    copies = parts.shape[0] // 16
    high = jnp.broadcast_to(target_high, (16, LOW))
    lhs = []
    for g in range(groups):
        mask = jnp.where(high == g, 1.0, 0.0).astype(BF16)
        lhs.append(parts * jnp.concatenate([mask] * copies, axis=0))
    return times_transposed(jnp.concatenate(lhs, axis=0), one_hot(target_low, LOW))


def kernel(
    sizes,
    x_hbm,
    w_hbm,
    dep_hbm,
    sp_hbm,
    count_hbm,
    turn_hbm,
    out_ref,
    count_ref,
    turn_ref,
    x,
    w,
    relay,
    dep,
    sp,
    hot,
    glhs,
    sent,
    acc,
    pay,
    inbox,
    w_recv,
    r_recv,
    p_recv,
    in_sem,
    w_send,
    p_send,
    e_send,
    z_send,
):
    n_panel, n_tile, n_lev = sizes
    fields, levels, cells = x.shape
    stencil = dep.shape[0]
    blocks, slots = sp.shape
    rows = fields * levels
    groups = cells // LOW
    share = cells // n_lev
    per_lev = share // LOW
    panel, tile, lev = (lax.axis_index(a) for a in ("panel", "tile", "lev"))
    shift_cell = cells.bit_length() - 1
    shift_low = LOW.bit_length() - 1
    at_slot = rows + 8
    size = rows + 16
    extras = blocks * size

    odd = lax.rem(tile, 2) == 1
    even = jnp.logical_not(odd)
    first = lev == 0
    lone = jnp.logical_and(even, first)
    helper = jnp.logical_and(odd, first)
    feeder = jnp.logical_and(even, jnp.logical_not(first))
    second = jnp.logical_and(even, lev == 1)
    other = jnp.logical_and(odd, jnp.logical_not(first))
    has_prev, has_next = tile > 0, tile < n_tile - 1
    whole = jnp.logical_and(has_prev, has_next)
    yes = tile >= 0
    next_panel, prev_panel = lax.rem(panel + 1, n_panel), lax.rem(panel + n_panel - 1, n_panel)
    prev_tile, next_tile = jnp.maximum(tile - 1, 0), jnp.minimum(tile + 1, n_tile - 1)
    toward = [{"tile": prev_tile}, {"tile": next_tile}, {"panel": prev_panel}, {"panel": next_panel}]
    sends_to = [has_prev, has_next, yes, yes]
    comes_from = [{"tile": next_tile}, {"tile": prev_tile}, {"panel": next_panel}, {"panel": prev_panel}]
    hears = [has_next, has_prev, yes, yes]
    from_even = [odd, odd, even, even]

    loads = [
        pltpu.make_async_copy(src, dst, in_sem.at[i])
        for i, (src, dst) in enumerate(
            (
                (sp_hbm, sp),
                (w_hbm, w.at[lev]),
                (count_hbm, count_ref),
                (turn_hbm, turn_ref),
                (dep_hbm, dep),
                (x_hbm, x),
            )
        )
    ]
    for load in loads:
        load.start()

    barrier = pltpu.get_barrier_semaphore()

    def greet(device):
        pl.semaphore_signal(barrier, inc=1, device_id=device, device_id_type=MESH)

    @pl.when(lone)
    def _():
        greet({"tile": next_tile})

    @pl.when(jnp.logical_not(lone))
    def _():
        for d in range(1, n_lev):
            greet({"lev": lax.rem(lev + d, n_lev)})
        for j in range(blocks):

            @pl.when(hears[j])
            def _(j=j):
                greet(comes_from[j])

                @pl.when(from_even[j])
                def _():
                    greet({**comes_from[j], "lev": jnp.where(first, 1, 0)})

    @pl.when(helper)
    def _():
        for t in range(1, n_lev):
            greet({"tile": prev_tile, "lev": t})
        for p in (prev_panel, next_panel):
            for t in range(2):
                greet({"panel": p, "tile": prev_tile, "lev": t})

        @pl.when(tile > 1)
        def _():
            greet({"tile": tile - 2})

    acc[...] = jnp.zeros_like(acc)
    for j in range(2):

        @pl.when(jnp.logical_not(hears[j]))
        def _(j=j):
            inbox[j * size : (j + 1) * size, :] = jnp.zeros((size, slots), F32)


    sent_blocks = 2 + has_prev.astype(I32) + has_next.astype(I32)
    more = jnp.where(lone, n_lev - 1, 0) + jnp.where(second, 1, 0)

    def weight_copy(d, dst, sem, device):
        return pltpu.make_async_remote_copy(
            src_ref=w.at[lev],
            dst_ref=dst.at[lev],
            send_sem=w_send,
            recv_sem=sem,
            device_id=device,
            device_id_type=MESH,
        )

    def enter():
        pl.semaphore_wait(barrier, n_lev - 1 + sent_blocks * (1 + more))
        for d in range(1, n_lev):
            indirect = jnp.logical_and(even, lev == n_lev - d)

            @pl.when(indirect)
            def _(d=d):
                weight_copy(d, relay, r_recv, {"tile": next_tile, "lev": 0}).start()

            @pl.when(jnp.logical_not(indirect))
            def _(d=d):
                weight_copy(d, w, w_recv.at[lev], {"lev": lax.rem(lev + d, n_lev)}).start()

    for load in loads[:2]:
        load.wait()

    @pl.when(lone)
    def _():
        enter()

    for load in loads[2:4]:
        load.wait()

    point = [sp[j : j + 1, :] for j in range(blocks)]
    cell_high = [(p & (cells - 1)) >> shift_low for p in point]
    stencil_of = [p >> shift_cell for p in point]
    lane = lax.broadcasted_iota(I32, (1, slots), 1)
    live = [lane < count_ref[j] for j in range(blocks)]
    for j in range(blocks):
        hot[:, j * slots : (j + 1) * slots] = one_hot(point[j] & (LOW - 1), slots)

    def slot_weights(parts):
        lhs = []
        for t in parts:
            for i in range(per_lev):
                w4 = w[t, :, i * LOW : (i + 1) * LOW]
                b1 = w4.astype(BF16).astype(F32)
                b2 = (w4 - b1).astype(BF16).astype(F32)
                lhs.append(
                    jnp.concatenate([b1, b2, w4 - b1 - b2, jnp.zeros_like(w4)], axis=0).astype(BF16)
                )
        found = jnp.dot(jnp.concatenate(lhs, axis=0), hot[...], preferred_element_type=F32)
        row16 = lax.broadcasted_iota(I32, (16, slots), 0)
        result = []
        for j in range(blocks):
            total = jnp.zeros((16, slots), F32)
            for n, t in enumerate(parts):
                for i in range(per_lev):
                    r = n * per_lev + i
                    piece = found[r * 16 : (r + 1) * 16, j * slots : (j + 1) * slots]
                    total = total + jnp.where(cell_high[j] == t * per_lev + i, piece, 0.0)
            own = (row16 & (stencil - 1)) == stencil_of[j]
            weight = jnp.sum(jnp.where(own, total, 0.0), axis=0, keepdims=True)
            result.append(jnp.where(live[j], weight, 0.0))
        return result

    def ahead(j, moved):
        if j >= 2:
            return {**toward[j], "tile": tile + moved}
        return {"tile": toward[j]["tile"] + moved}

    def block_copy(j):
        moved = jnp.where(helper, 1, 0) if j == 1 else (jnp.where(lone, 1, 0) if j >= 2 else 0)
        at = j * size if j == 0 else pl.multiple_of(j * size + moved * (blocks * (size + 8) - size), 8)
        return pltpu.make_async_remote_copy(
            src_ref=pay.at[j],
            dst_ref=inbox.at[pl.ds(at, size)],
            send_sem=p_send,
            recv_sem=p_recv.at[moved],
            device_id=ahead(j, moved),
            device_id_type=MESH,
        )

    def extra_copy(j, level):
        moved = jnp.where(second, 1, 0) if level == 0 and j >= 2 else 0
        return pltpu.make_async_remote_copy(
            src_ref=pay.at[j, pl.ds(at_slot, 8)],
            dst_ref=inbox.at[pl.ds(extras + 8 * j, 8)],
            send_sem=e_send,
            recv_sem=p_recv.at[moved],
            device_id={**ahead(j, moved), "lev": level},
            device_id_type=MESH,
        )

    def send_blocks():
        for j in (1, 0, 2, 3):

            @pl.when(sends_to[j])
            def _(j=j):
                block_copy(j).start()

    for j, weight in enumerate(slot_weights([lev])):
        pay[j, at_slot:, :] = jnp.broadcast_to(weight, (8, slots))

    @pl.when(lone)
    def _():
        for t in range(1, n_lev):
            for j in (1, 0, 2, 3):

                @pl.when(sends_to[j])
                def _(j=j, t=t):
                    extra_copy(j, t).start()

    for load in loads[4:]:
        load.wait()

    height = 2 * rows + 16
    for g in range(groups):
        part = x[:, :, g * LOW : (g + 1) * LOW].reshape(rows, LOW)
        d4 = dep[:, g * LOW : (g + 1) * LOW]
        d8 = jnp.concatenate([d4 >> shift_low, d4 & (LOW - 1)], axis=0).astype(F32)
        d16 = jnp.concatenate([d8, jnp.zeros((8, LOW), F32)], axis=0).astype(BF16)
        glhs[g * height : g * height + 2 * rows, :] = split_rows(part)
        glhs[g * height + 2 * rows : (g + 1) * height, :] = d16
    row8 = lax.broadcasted_iota(I32, (8, slots), 0)
    for n in range(blocks * slots // LOW):
        found = jnp.dot(glhs[...], hot[:, n * LOW : (n + 1) * LOW], preferred_element_type=F32)
        for i in range(LOW // slots):
            j = n * (LOW // slots) + i
            total = jnp.zeros((height, slots), F32)
            for g in range(groups):
                piece = found[g * height : (g + 1) * height, i * slots : (i + 1) * slots]
                total = total + jnp.where(cell_high[j] == g, piece, 0.0)
            value = total[:rows] + total[rows : 2 * rows]
            if j >= 2:
                code = turn_ref[j - 2]
                cosine = jnp.where(code == 0, 1.0, 0.0) - jnp.where(code == 2, 1.0, 0.0)
                sine = jnp.where(code == 1, 1.0, 0.0) - jnp.where(code == 3, 1.0, 0.0)
                zonal, merid = value[:levels], value[levels : 2 * levels]
                value = jnp.concatenate(
                    [
                        cosine * zonal + sine * merid,
                        cosine * merid - sine * zonal,
                        value[2 * levels :],
                    ],
                    axis=0,
                )
            scale = jnp.where(row8 < stencil, float(LOW), 1.0)
            own = (row8 & (stencil - 1)) == stencil_of[j]
            target = jnp.sum(
                jnp.where(own, total[2 * rows : 2 * rows + 8] * scale, 0.0), axis=0, keepdims=True
            )
            pay[j, 0:rows, :] = value
            pay[j, rows:at_slot, :] = jnp.broadcast_to(target, (8, slots))

    @pl.when(lone)
    def _():
        send_blocks()

    number = lax.broadcasted_iota(I32, (stencil * groups, slots), 0)
    marks = [
        jnp.where((number == (point[j] >> shift_low)) & live[j], 1.0, 0.0).astype(BF16)
        for j in range(blocks)
    ]
    sent[...] = times_transposed(jnp.concatenate(marks, axis=1), hot[...])

    def segment(t):
        result = None
        for i in range(per_lev):
            at = pl.ds(pl.multiple_of(t * share + i * LOW, LOW), LOW)
            part = x[:, :, at].reshape(rows, LOW)
            for k in range(stencil):
                weight = w[t, k : k + 1, i * LOW : (i + 1) * LOW]
                landing = dep[k : k + 1, at]
                gone = sent[pl.ds(k * groups + t * per_lev + i, 1), :]
                high = jnp.where(gone > 0.5, groups, landing >> shift_low)
                term = spread(part * weight, high, landing & (LOW - 1), groups)
                result = term if result is None else result + term
        return result

    order = [
        lev,
        jnp.where(first, 1, 1 + lax.rem(lev, 3)),
        jnp.where(first, 2, 1 + lax.rem(lev + 1, 3)),
        jnp.where(first, 3, 0),
    ]

    def await_bytes(ref, sem):
        pltpu.make_async_copy(ref, ref, sem).wait()

    def add_weights(parts):
        weights = slot_weights(parts)
        for j in range(blocks):
            pay[j, at_slot:, :] += jnp.broadcast_to(weights[j], (8, slots))
        send_blocks()

    def to_lone(src, dst, send_sem, recv_sem):
        return pltpu.make_async_remote_copy(
            src_ref=src,
            dst_ref=dst,
            send_sem=send_sem,
            recv_sem=recv_sem,
            device_id={"tile": prev_tile},
            device_id_type=MESH,
        )

    others = pl.ds(1, n_lev - 1)
    relay_copy = to_lone(relay.at[others], w.at[others], z_send.at[0], w_recv.at[0])
    aside = blocks * (size + 8)
    last_two = pl.ds(2 * size, 2 * size)
    last_extras = pl.ds(extras + 16, 16)
    pass_one = to_lone(inbox.at[pl.ds(aside, size)], inbox.at[pl.ds(size, size)], z_send.at[1], p_recv.at[0])
    pass_two = to_lone(
        inbox.at[pl.ds(aside + size, 2 * size)], inbox.at[last_two], z_send.at[1], p_recv.at[0]
    )
    pass_extras = to_lone(inbox.at[last_extras], inbox.at[last_extras], z_send.at[1], p_recv.at[0])
    passed = 3 * size + 16, 2 * size + 16

    def both(*conditions):
        return functools.reduce(jnp.logical_and, conditions)

    soon = both(feeder, lax.rem(panel, 2) == 0)

    def step(i, carry):
        @pl.when(i == jnp.where(helper, 3, jnp.where(other, 1, jnp.where(feeder, 0, -1))))
        def _():
            enter()

        when = (
            jnp.where(lone, -1, 1),
            jnp.where(lone, -1, jnp.where(feeder, 1, 2)),
            jnp.where(lone, -1, jnp.where(soon, 4, 3)),
        )
        for n in range(3):

            @pl.when(i == when[n])
            def _(n=n):
                await_bytes(w.at[order[n + 1]], w_recv.at[order[n + 1]])

        @pl.when(both(odd, i == when[2]))
        def _():
            add_weights(order[1:])

        @pl.when(both(feeder, i == 1))
        def _():
            add_weights(order[1:3])

            @pl.when(second)
            def _():
                for j in range(blocks):

                    @pl.when(sends_to[j])
                    def _(j=j):
                        extra_copy(j, 0).start()

        @pl.when(both(helper, i == 3))
        def _():
            await_bytes(relay.at[others], r_recv)
            relay_copy.start()

        @pl.when(both(lone, i == 1))
        def _():
            await_bytes(w.at[others], w_recv.at[0])

        @pl.when(both(helper, i == 4, tile > 1))
        def _():
            await_bytes(inbox.at[pl.ds(0, passed[0])], p_recv.at[1])
            pass_one.start()

        @pl.when(both(helper, i == 4, tile == 1))
        def _():
            await_bytes(inbox.at[pl.ds(0, passed[1])], p_recv.at[1])

        @pl.when(both(helper, i == 4))
        def _():
            pass_two.start()
            pass_extras.start()

        arriving = i == jnp.where(soon, 3, 4)

        @pl.when(jnp.logical_not(arriving))
        def _():
            k = jnp.minimum(i, 3)
            t = jnp.where(
                k == 0, order[0], jnp.where(k == 1, order[1], jnp.where(k == 2, order[2], order[3]))
            )
            acc[...] += segment(t)

        @pl.when(arriving)
        def _():
            await_bytes(w.at[others], w_send)
            for n, edge in ((blocks, whole), (blocks - 1, jnp.logical_not(whole))):

                @pl.when(edge)
                def _(n=n):
                    await_bytes(pay.at[pl.ds(0, n)], p_send)

                for role, times in ((lone, n_lev - 1), (second, 1)):

                    @pl.when(both(role, edge))
                    def _(n=n, times=times):
                        await_bytes(inbox.at[pl.ds(0, 8 * n * times)], e_send)

            @pl.when(helper)
            def _():
                await_bytes(relay.at[others], z_send.at[0])

            for edge, n, m in (
                (whole, blocks, 2),
                (jnp.logical_not(has_prev), blocks - 1, 2),
                (jnp.logical_not(has_next), blocks - 1, 1),
            ):

                @pl.when(edge)
                def _(n=n, m=m):
                    await_bytes(inbox.at[pl.ds(0, n * size + 8 * m)], p_recv.at[0])

            for j in range(blocks):

                @pl.when(jnp.logical_and(hears[j], from_even[j]))
                def _(j=j):
                    inbox[j * size + at_slot : (j + 1) * size, :] += inbox[
                        extras + 8 * j : extras + 8 * (j + 1), :
                    ]

            result = acc[...]
            for pair in ((0, 2), (1, 3)):
                value = jnp.concatenate(
                    [
                        inbox[j * size : j * size + rows, :]
                        * inbox[j * size + at_slot : j * size + at_slot + 1, :]
                        for j in pair
                    ],
                    axis=1,
                )
                landing = jnp.concatenate(
                    [inbox[j * size + rows : j * size + rows + 1, :] for j in pair], axis=1
                ).astype(I32)
                result = result + spread(value, landing >> shift_low, landing & (LOW - 1), groups)
            acc[...] = result

        return carry

    lax.fori_loop(0, 5, step, 0)

    result = acc
    for g in range(groups):
        top = g * 2 * rows
        out_ref[:, :, g * LOW : (g + 1) * LOW] = (
            result[top : top + rows, :] + result[top + rows : top + 2 * rows, :]
        ).reshape(fields, levels, LOW)

    for edge, n in ((tile > 1, passed[0]), (tile == 1, passed[1])):

        @pl.when(both(helper, edge))
        def _(n=n):
            await_bytes(inbox.at[pl.ds(0, n)], z_send.at[1])


def scoped(sizes, *refs):
    dma = pltpu.SemaphoreType.DMA
    pl.run_scoped(functools.partial(kernel, sizes, *refs), dma((6,)), dma, dma, dma, dma((2,)))


def body(sizes, adjoint_new, weights, departure, send_point, block_count, rotation):
    fields, levels, cells = adjoint_new.shape
    stencil = departure.shape[0]
    blocks, slots = send_point.shape
    rows = fields * levels
    groups = cells // LOW
    n_lev = sizes[2]
    hbm = pl.BlockSpec(memory_space=pltpu.HBM)
    args = (adjoint_new, weights, departure, send_point, block_count.reshape(-1), rotation.reshape(-1))
    return pl.pallas_call(
        functools.partial(scoped, sizes),
        out_shape=pltpu.VMEM(adjoint_new.shape, F32),
        in_specs=[hbm] * len(args),
        out_specs=pl.BlockSpec(memory_space=pltpu.VMEM),
        scratch_shapes=[
            pltpu.SMEM((blocks,), I32),
            pltpu.SMEM((rotation.shape[0],), I32),
            pltpu.VMEM((fields, levels, cells), F32),
            pltpu.VMEM((n_lev, stencil, cells // n_lev), F32),
            pltpu.VMEM((n_lev, stencil, cells // n_lev), F32),
            pltpu.VMEM((stencil, cells), I32),
            pltpu.VMEM((blocks, slots), I32),
            pltpu.VMEM((LOW, blocks * slots), BF16),
            pltpu.VMEM((groups * (2 * rows + 16), LOW), BF16),
            pltpu.VMEM((stencil * groups, LOW), F32),
            pltpu.VMEM((groups * 2 * rows, LOW), F32),
            pltpu.VMEM((blocks, rows + 16, slots), F32),
            pltpu.VMEM((blocks * (rows + 24) + 3 * (rows + 16), slots), F32),
            pltpu.SemaphoreType.DMA((n_lev,)),
            pltpu.SemaphoreType.DMA,
            pltpu.SemaphoreType.DMA((2,)),
        ],
        compiler_params=pltpu.CompilerParams(
            collective_id=0, has_side_effects=True, vmem_limit_bytes=16 * 1024 * 1024
        ),
    )(*(pltpu.with_memory_space_constraint(a, pltpu.HBM) for a in args))


def solution(mesh):
    sizes = tuple(mesh.shape[a] for a in ("panel", "tile", "lev"))
    return jax.shard_map(
        functools.partial(body, sizes),
        mesh=mesh,
        in_specs=(
            P(None, "lev", ("panel", "tile")),
            P(None, ("panel", "tile", "lev")),
            P(None, ("panel", "tile")),
            P(None, ("panel", "tile")),
            P(None, ("panel", "tile")),
            P(None, ("panel", "tile")),
        ),
        out_specs=P(None, "lev", ("panel", "tile")),
        check_vma=False,
    )
```

```python
import functools

import jax
import jax.numpy as jnp
from jax import lax
from jax.experimental import pallas as pl
from jax.experimental.pallas import tpu as pltpu
from jax.sharding import PartitionSpec as P

MESH = pl.DeviceIdType.MESH
LOW = 256
F32, BF16, I32 = jnp.float32, jnp.bfloat16, jnp.int32


def split_rows(value):
    high = value.astype(BF16).astype(F32)
    return jnp.concatenate([high, value - high], axis=0).astype(BF16)


def one_hot(low, columns):
    rows = lax.broadcasted_iota(I32, (LOW, columns), 0)
    return jnp.where(rows == low, 1.0, 0.0).astype(BF16)


def times_transposed(lhs, rhs):
    return lax.dot_general(lhs, rhs, (((1,), (1,)), ((), ())), preferred_element_type=F32)


def spread(value, target_high, target_low, groups):
    parts = split_rows(value)
    copies = parts.shape[0] // 16
    high = jnp.broadcast_to(target_high, (16, LOW))
    lhs = []
    for g in range(groups):
        mask = jnp.where(high == g, 1.0, 0.0).astype(BF16)
        lhs.append(parts * jnp.concatenate([mask] * copies, axis=0))
    return times_transposed(jnp.concatenate(lhs, axis=0), one_hot(target_low, LOW))


def kernel(
    sizes,
    x_hbm,
    w_hbm,
    dep_hbm,
    sp_hbm,
    count_hbm,
    turn_hbm,
    out_ref,
    count_ref,
    turn_ref,
    x,
    w,
    relay,
    dep,
    sp,
    hot,
    glhs,
    sent,
    acc,
    pay,
    inbox,
    w_recv,
    r_recv,
    p_recv,
    in_sem,
    w_send,
    p_send,
    e_send,
    z_send,
):
    n_panel, n_tile, n_lev = sizes
    fields, levels, cells = x.shape
    stencil = dep.shape[0]
    blocks, slots = sp.shape
    rows = fields * levels
    groups = cells // LOW
    share = cells // n_lev
    per_lev = share // LOW
    panel, tile, lev = (lax.axis_index(a) for a in ("panel", "tile", "lev"))
    shift_cell = cells.bit_length() - 1
    shift_low = LOW.bit_length() - 1
    at_slot = rows + 8
    size = rows + 16
    extras = blocks * size

    odd = lax.rem(tile, 2) == 1
    even = jnp.logical_not(odd)
    first = lev == 0
    lone = jnp.logical_and(even, first)
    helper = jnp.logical_and(odd, first)
    feeder = jnp.logical_and(even, jnp.logical_not(first))
    second = jnp.logical_and(even, lev == 1)
    other = jnp.logical_and(odd, jnp.logical_not(first))
    even_panel = lax.rem(panel, 2) == 0
    odd_panel = jnp.logical_not(even_panel)
    has_prev, has_next = tile > 0, tile < n_tile - 1
    whole = jnp.logical_and(has_prev, has_next)
    yes = tile >= 0
    next_panel, prev_panel = lax.rem(panel + 1, n_panel), lax.rem(panel + n_panel - 1, n_panel)
    prev_tile, next_tile = jnp.maximum(tile - 1, 0), jnp.minimum(tile + 1, n_tile - 1)
    toward = [{"tile": prev_tile}, {"tile": next_tile}, {"panel": prev_panel}, {"panel": next_panel}]
    sends_to = [has_prev, has_next, yes, yes]
    comes_from = [{"tile": next_tile}, {"tile": prev_tile}, {"panel": next_panel}, {"panel": prev_panel}]
    hears = [has_next, has_prev, yes, yes]
    from_even = [odd, odd, even, even]

    loads = [
        pltpu.make_async_copy(src, dst, in_sem.at[i])
        for i, (src, dst) in enumerate(
            (
                (sp_hbm, sp),
                (w_hbm, w.at[lev]),
                (count_hbm, count_ref),
                (turn_hbm, turn_ref),
                (dep_hbm, dep),
                (x_hbm, x),
            )
        )
    ]
    for load in loads:
        load.start()

    barrier = pltpu.get_barrier_semaphore()

    def greet(device):
        pl.semaphore_signal(barrier, inc=1, device_id=device, device_id_type=MESH)

    @pl.when(lone)
    def _():
        greet({"tile": next_tile})

        @pl.when(odd_panel)
        def _():
            for p in (prev_panel, next_panel):
                for t in range(2):
                    greet({"panel": p, "lev": t})

    @pl.when(jnp.logical_not(lone))
    def _():
        for d in range(1, n_lev):
            greet({"lev": lax.rem(lev + d, n_lev)})
        for j in range(blocks):

            @pl.when(hears[j])
            def _(j=j):
                greet(comes_from[j])

                @pl.when(from_even[j])
                def _():
                    greet({**comes_from[j], "lev": jnp.where(first, 1, 0)})

    @pl.when(helper)
    def _():
        for t in range(1, n_lev):
            greet({"tile": prev_tile, "lev": t})

        @pl.when(even_panel)
        def _():
            for p in (prev_panel, next_panel):
                for t in range(2):
                    greet({"panel": p, "tile": prev_tile, "lev": t})

        @pl.when(tile > 1)
        def _():
            greet({"tile": tile - 2})

    acc[...] = jnp.zeros_like(acc)
    for j in range(2):

        @pl.when(jnp.logical_not(hears[j]))
        def _(j=j):
            inbox[j * size : (j + 1) * size, :] = jnp.zeros((size, slots), F32)


    sent_blocks = 2 + has_prev.astype(I32) + has_next.astype(I32)
    more = jnp.where(lone, n_lev - 1, 0) + jnp.where(second, 1, 0)

    def weight_copy(d, dst, sem, device):
        return pltpu.make_async_remote_copy(
            src_ref=w.at[lev],
            dst_ref=dst.at[lev],
            send_sem=w_send,
            recv_sem=sem,
            device_id=device,
            device_id_type=MESH,
        )

    def enter():
        pl.semaphore_wait(barrier, n_lev - 1 + sent_blocks * (1 + more))
        for d in range(1, n_lev):
            indirect = jnp.logical_and(even, lev == n_lev - d)

            @pl.when(indirect)
            def _(d=d):
                weight_copy(d, relay, r_recv, {"tile": next_tile, "lev": 0}).start()

            @pl.when(jnp.logical_not(indirect))
            def _(d=d):
                weight_copy(d, w, w_recv.at[lev], {"lev": lax.rem(lev + d, n_lev)}).start()

    for load in loads[:2]:
        load.wait()

    @pl.when(lone)
    def _():
        enter()

    for load in loads[2:4]:
        load.wait()

    point = [sp[j : j + 1, :] for j in range(blocks)]
    cell_high = [(p & (cells - 1)) >> shift_low for p in point]
    stencil_of = [p >> shift_cell for p in point]
    lane = lax.broadcasted_iota(I32, (1, slots), 1)
    live = [lane < count_ref[j] for j in range(blocks)]
    for j in range(blocks):
        hot[:, j * slots : (j + 1) * slots] = one_hot(point[j] & (LOW - 1), slots)

    def slot_weights(parts):
        lhs = []
        for t in parts:
            for i in range(per_lev):
                w4 = w[t, :, i * LOW : (i + 1) * LOW]
                b1 = w4.astype(BF16).astype(F32)
                b2 = (w4 - b1).astype(BF16).astype(F32)
                lhs.append(
                    jnp.concatenate([b1, b2, w4 - b1 - b2, jnp.zeros_like(w4)], axis=0).astype(BF16)
                )
        found = jnp.dot(jnp.concatenate(lhs, axis=0), hot[...], preferred_element_type=F32)
        row16 = lax.broadcasted_iota(I32, (16, slots), 0)
        result = []
        for j in range(blocks):
            total = jnp.zeros((16, slots), F32)
            for n, t in enumerate(parts):
                for i in range(per_lev):
                    r = n * per_lev + i
                    piece = found[r * 16 : (r + 1) * 16, j * slots : (j + 1) * slots]
                    total = total + jnp.where(cell_high[j] == t * per_lev + i, piece, 0.0)
            own = (row16 & (stencil - 1)) == stencil_of[j]
            weight = jnp.sum(jnp.where(own, total, 0.0), axis=0, keepdims=True)
            result.append(jnp.where(live[j], weight, 0.0))
        return result

    aslant = jnp.logical_and(lone, odd_panel)

    def ahead(j, moved):
        if j >= 2:
            return {**toward[j], "tile": tile + moved}
        return {"tile": toward[j]["tile"] + moved}

    def block_copy(j):
        moved = jnp.where(helper, 1, 0) if j == 1 else (jnp.where(aslant, 1, 0) if j >= 2 else 0)
        at = j * size if j == 0 else pl.multiple_of(j * size + moved * (blocks * (size + 8) - size), 8)
        return pltpu.make_async_remote_copy(
            src_ref=pay.at[j],
            dst_ref=inbox.at[pl.ds(at, size)],
            send_sem=p_send,
            recv_sem=p_recv.at[moved],
            device_id=ahead(j, moved),
            device_id_type=MESH,
        )

    def extra_copy(j, level):
        moved = jnp.where(jnp.logical_and(second, odd_panel), 1, 0) if level == 0 and j >= 2 else 0
        return pltpu.make_async_remote_copy(
            src_ref=pay.at[j, pl.ds(at_slot, 8)],
            dst_ref=inbox.at[pl.ds(extras + 8 * j, 8)],
            send_sem=e_send,
            recv_sem=p_recv.at[moved],
            device_id={**ahead(j, moved), "lev": level},
            device_id_type=MESH,
        )

    def send_blocks():
        for j in (1, 0, 2, 3):

            @pl.when(sends_to[j])
            def _(j=j):
                block_copy(j).start()

    for j, weight in enumerate(slot_weights([lev])):
        pay[j, at_slot:, :] = jnp.broadcast_to(weight, (8, slots))

    @pl.when(lone)
    def _():
        for t in range(1, n_lev):
            for j in (1, 0, 2, 3):

                @pl.when(sends_to[j])
                def _(j=j, t=t):
                    extra_copy(j, t).start()

    for load in loads[4:]:
        load.wait()

    height = 2 * rows + 16
    for g in range(groups):
        part = x[:, :, g * LOW : (g + 1) * LOW].reshape(rows, LOW)
        d4 = dep[:, g * LOW : (g + 1) * LOW]
        d8 = jnp.concatenate([d4 >> shift_low, d4 & (LOW - 1)], axis=0).astype(F32)
        d16 = jnp.concatenate([d8, jnp.zeros((8, LOW), F32)], axis=0).astype(BF16)
        glhs[g * height : g * height + 2 * rows, :] = split_rows(part)
        glhs[g * height + 2 * rows : (g + 1) * height, :] = d16
    row8 = lax.broadcasted_iota(I32, (8, slots), 0)
    for n in range(blocks * slots // LOW):
        found = jnp.dot(glhs[...], hot[:, n * LOW : (n + 1) * LOW], preferred_element_type=F32)
        for i in range(LOW // slots):
            j = n * (LOW // slots) + i
            total = jnp.zeros((height, slots), F32)
            for g in range(groups):
                piece = found[g * height : (g + 1) * height, i * slots : (i + 1) * slots]
                total = total + jnp.where(cell_high[j] == g, piece, 0.0)
            value = total[:rows] + total[rows : 2 * rows]
            if j >= 2:
                code = turn_ref[j - 2]
                cosine = jnp.where(code == 0, 1.0, 0.0) - jnp.where(code == 2, 1.0, 0.0)
                sine = jnp.where(code == 1, 1.0, 0.0) - jnp.where(code == 3, 1.0, 0.0)
                zonal, merid = value[:levels], value[levels : 2 * levels]
                value = jnp.concatenate(
                    [
                        cosine * zonal + sine * merid,
                        cosine * merid - sine * zonal,
                        value[2 * levels :],
                    ],
                    axis=0,
                )
            scale = jnp.where(row8 < stencil, float(LOW), 1.0)
            own = (row8 & (stencil - 1)) == stencil_of[j]
            target = jnp.sum(
                jnp.where(own, total[2 * rows : 2 * rows + 8] * scale, 0.0), axis=0, keepdims=True
            )
            pay[j, 0:rows, :] = value
            pay[j, rows:at_slot, :] = jnp.broadcast_to(target, (8, slots))

    @pl.when(lone)
    def _():
        send_blocks()

    number = lax.broadcasted_iota(I32, (stencil * groups, slots), 0)
    marks = [
        jnp.where((number == (point[j] >> shift_low)) & live[j], 1.0, 0.0).astype(BF16)
        for j in range(blocks)
    ]
    sent[...] = times_transposed(jnp.concatenate(marks, axis=1), hot[...])

    def segment(t):
        result = None
        for i in range(per_lev):
            at = pl.ds(pl.multiple_of(t * share + i * LOW, LOW), LOW)
            part = x[:, :, at].reshape(rows, LOW)
            for k in range(stencil):
                weight = w[t, k : k + 1, i * LOW : (i + 1) * LOW]
                landing = dep[k : k + 1, at]
                gone = sent[pl.ds(k * groups + t * per_lev + i, 1), :]
                high = jnp.where(gone > 0.5, groups, landing >> shift_low)
                term = spread(part * weight, high, landing & (LOW - 1), groups)
                result = term if result is None else result + term
        return result

    order = [
        lev,
        jnp.where(first, 1, 1 + lax.rem(lev, 3)),
        jnp.where(first, 2, 1 + lax.rem(lev + 1, 3)),
        jnp.where(first, 3, 0),
    ]

    def await_bytes(ref, sem):
        pltpu.make_async_copy(ref, ref, sem).wait()

    def add_weights(parts):
        weights = slot_weights(parts)
        for j in range(blocks):
            pay[j, at_slot:, :] += jnp.broadcast_to(weights[j], (8, slots))
        send_blocks()

    def to_lone(src, dst, send_sem, recv_sem):
        return pltpu.make_async_remote_copy(
            src_ref=src,
            dst_ref=dst,
            send_sem=send_sem,
            recv_sem=recv_sem,
            device_id={"tile": prev_tile},
            device_id_type=MESH,
        )

    others = pl.ds(1, n_lev - 1)
    relay_copy = to_lone(relay.at[others], w.at[others], z_send.at[0], w_recv.at[0])
    aside = blocks * (size + 8)
    last_two = pl.ds(2 * size, 2 * size)
    last_extras = pl.ds(extras + 16, 16)
    pass_one = to_lone(inbox.at[pl.ds(aside, size)], inbox.at[pl.ds(size, size)], z_send.at[1], p_recv.at[0])
    pass_two = to_lone(
        inbox.at[pl.ds(aside + size, 2 * size)], inbox.at[last_two], z_send.at[1], p_recv.at[0]
    )
    pass_extras = to_lone(inbox.at[last_extras], inbox.at[last_extras], z_send.at[1], p_recv.at[0])
    passed = [
        (functools.reduce(jnp.logical_and, (helper, *case)), rows_passed)
        for case, rows_passed in (
            ((even_panel, tile > 1), 3 * size + 16),
            ((even_panel, tile == 1), 2 * size + 16),
            ((odd_panel, tile > 1), size),
        )
    ]

    def both(*conditions):
        return functools.reduce(jnp.logical_and, conditions)

    soon = both(feeder, even_panel, lax.rem(tile, 4) == 0)

    def step(i, carry):
        @pl.when(i == jnp.where(helper, 3, jnp.where(other, 1, jnp.where(feeder, 0, -1))))
        def _():
            enter()

        when = (
            jnp.where(lone, -1, 1),
            jnp.where(lone, -1, jnp.where(feeder, 1, 2)),
            jnp.where(lone, -1, jnp.where(soon, 4, 3)),
        )
        for n in range(3):

            @pl.when(i == when[n])
            def _(n=n):
                await_bytes(w.at[order[n + 1]], w_recv.at[order[n + 1]])

        @pl.when(both(odd, i == when[2]))
        def _():
            add_weights(order[1:])

        @pl.when(both(feeder, i == 1))
        def _():
            add_weights(order[1:3])

            @pl.when(second)
            def _():
                for j in range(blocks):

                    @pl.when(sends_to[j])
                    def _(j=j):
                        extra_copy(j, 0).start()

        @pl.when(both(helper, i == 3))
        def _():
            await_bytes(relay.at[others], r_recv)
            relay_copy.start()

        @pl.when(both(lone, i == 1))
        def _():
            await_bytes(w.at[others], w_recv.at[0])

        for case, n in passed:

            @pl.when(both(case, i == 4))
            def _(n=n):
                await_bytes(inbox.at[pl.ds(0, n)], p_recv.at[1])

        @pl.when(both(helper, i == 4))
        def _():
            @pl.when(tile > 1)
            def _():
                pass_one.start()

            @pl.when(even_panel)
            def _():
                pass_two.start()
                pass_extras.start()

        arriving = i == jnp.where(soon, 3, 4)

        @pl.when(jnp.logical_not(arriving))
        def _():
            k = jnp.minimum(i, 3)
            t = jnp.where(
                k == 0, order[0], jnp.where(k == 1, order[1], jnp.where(k == 2, order[2], order[3]))
            )
            acc[...] += segment(t)

        @pl.when(arriving)
        def _():
            await_bytes(w.at[others], w_send)
            for n, edge in ((blocks, whole), (blocks - 1, jnp.logical_not(whole))):

                @pl.when(edge)
                def _(n=n):
                    await_bytes(pay.at[pl.ds(0, n)], p_send)

                for role, times in ((lone, n_lev - 1), (second, 1)):

                    @pl.when(both(role, edge))
                    def _(n=n, times=times):
                        await_bytes(inbox.at[pl.ds(0, 8 * n * times)], e_send)

            @pl.when(helper)
            def _():
                await_bytes(relay.at[others], z_send.at[0])

            for edge, n, m in (
                (whole, blocks, 2),
                (jnp.logical_not(has_prev), blocks - 1, 2),
                (jnp.logical_not(has_next), blocks - 1, 1),
            ):

                @pl.when(edge)
                def _(n=n, m=m):
                    await_bytes(inbox.at[pl.ds(0, n * size + 8 * m)], p_recv.at[0])

            for j in range(blocks):

                @pl.when(jnp.logical_and(hears[j], from_even[j]))
                def _(j=j):
                    inbox[j * size + at_slot : (j + 1) * size, :] += inbox[
                        extras + 8 * j : extras + 8 * (j + 1), :
                    ]

            result = acc[...]
            for pair in ((0, 2), (1, 3)):
                value = jnp.concatenate(
                    [
                        inbox[j * size : j * size + rows, :]
                        * inbox[j * size + at_slot : j * size + at_slot + 1, :]
                        for j in pair
                    ],
                    axis=1,
                )
                landing = jnp.concatenate(
                    [inbox[j * size + rows : j * size + rows + 1, :] for j in pair], axis=1
                ).astype(I32)
                result = result + spread(value, landing >> shift_low, landing & (LOW - 1), groups)
            acc[...] = result

        return carry

    lax.fori_loop(0, 5, step, 0)

    result = acc
    for g in range(groups):
        top = g * 2 * rows
        out_ref[:, :, g * LOW : (g + 1) * LOW] = (
            result[top : top + rows, :] + result[top + rows : top + 2 * rows, :]
        ).reshape(fields, levels, LOW)

    for case, n in passed:

        @pl.when(case)
        def _(n=n):
            await_bytes(inbox.at[pl.ds(0, n)], z_send.at[1])


def scoped(sizes, *refs):
    dma = pltpu.SemaphoreType.DMA
    pl.run_scoped(functools.partial(kernel, sizes, *refs), dma((6,)), dma, dma, dma, dma((2,)))


def body(sizes, adjoint_new, weights, departure, send_point, block_count, rotation):
    fields, levels, cells = adjoint_new.shape
    stencil = departure.shape[0]
    blocks, slots = send_point.shape
    rows = fields * levels
    groups = cells // LOW
    n_lev = sizes[2]
    hbm = pl.BlockSpec(memory_space=pltpu.HBM)
    args = (adjoint_new, weights, departure, send_point, block_count.reshape(-1), rotation.reshape(-1))
    return pl.pallas_call(
        functools.partial(scoped, sizes),
        out_shape=pltpu.VMEM(adjoint_new.shape, F32),
        in_specs=[hbm] * len(args),
        out_specs=pl.BlockSpec(memory_space=pltpu.VMEM),
        scratch_shapes=[
            pltpu.SMEM((blocks,), I32),
            pltpu.SMEM((rotation.shape[0],), I32),
            pltpu.VMEM((fields, levels, cells), F32),
            pltpu.VMEM((n_lev, stencil, cells // n_lev), F32),
            pltpu.VMEM((n_lev, stencil, cells // n_lev), F32),
            pltpu.VMEM((stencil, cells), I32),
            pltpu.VMEM((blocks, slots), I32),
            pltpu.VMEM((LOW, blocks * slots), BF16),
            pltpu.VMEM((groups * (2 * rows + 16), LOW), BF16),
            pltpu.VMEM((stencil * groups, LOW), F32),
            pltpu.VMEM((groups * 2 * rows, LOW), F32),
            pltpu.VMEM((blocks, rows + 16, slots), F32),
            pltpu.VMEM((blocks * (rows + 24) + 3 * (rows + 16), slots), F32),
            pltpu.SemaphoreType.DMA((n_lev,)),
            pltpu.SemaphoreType.DMA,
            pltpu.SemaphoreType.DMA((2,)),
        ],
        compiler_params=pltpu.CompilerParams(
            collective_id=0, has_side_effects=True, vmem_limit_bytes=16 * 1024 * 1024
        ),
    )(*(pltpu.with_memory_space_constraint(a, pltpu.HBM) for a in args))


def solution(mesh):
    sizes = tuple(mesh.shape[a] for a in ("panel", "tile", "lev"))
    return jax.shard_map(
        functools.partial(body, sizes),
        mesh=mesh,
        in_specs=(
            P(None, "lev", ("panel", "tile")),
            P(None, ("panel", "tile", "lev")),
            P(None, ("panel", "tile")),
            P(None, ("panel", "tile")),
            P(None, ("panel", "tile")),
            P(None, ("panel", "tile")),
        ),
        out_specs=P(None, "lev", ("panel", "tile")),
        check_vma=False,
    )
```

```python
import functools

import jax
import jax.numpy as jnp
from jax import lax
from jax.experimental import pallas as pl
from jax.experimental.pallas import tpu as pltpu
from jax.sharding import PartitionSpec as P

MESH = pl.DeviceIdType.MESH
LOW = 256
F32, BF16, I32 = jnp.float32, jnp.bfloat16, jnp.int32


def split_rows(value):
    high = value.astype(BF16).astype(F32)
    return jnp.concatenate([high, value - high], axis=0).astype(BF16)


def one_hot(low, columns):
    rows = lax.broadcasted_iota(I32, (LOW, columns), 0)
    return jnp.where(rows == low, 1.0, 0.0).astype(BF16)


def times_transposed(lhs, rhs):
    return lax.dot_general(lhs, rhs, (((1,), (1,)), ((), ())), preferred_element_type=F32)


def spread(value, target_high, target_low, groups):
    parts = split_rows(value)
    copies = parts.shape[0] // 16
    high = jnp.broadcast_to(target_high, (16, LOW))
    lhs = []
    for g in range(groups):
        mask = jnp.where(high == g, 1.0, 0.0).astype(BF16)
        lhs.append(parts * jnp.concatenate([mask] * copies, axis=0))
    return times_transposed(jnp.concatenate(lhs, axis=0), one_hot(target_low, LOW))


def kernel(
    sizes,
    x_hbm,
    w_hbm,
    dep_hbm,
    sp_hbm,
    count_hbm,
    turn_hbm,
    out_ref,
    count_ref,
    turn_ref,
    x,
    w,
    relay,
    dep,
    sp,
    hot,
    glhs,
    sent,
    acc,
    pay,
    mine,
    inbox,
    w_recv,
    r_recv,
    p_recv,
    in_sem,
    w_send,
    p_send,
    e_send,
    z_send,
):
    n_panel, n_tile, n_lev = sizes
    fields, levels, cells = x.shape
    stencil = dep.shape[0]
    blocks, slots = sp.shape
    rows = fields * levels
    groups = cells // LOW
    share = cells // n_lev
    per_lev = share // LOW
    panel, tile, lev = (lax.axis_index(a) for a in ("panel", "tile", "lev"))
    shift_cell = cells.bit_length() - 1
    shift_low = LOW.bit_length() - 1
    at_slot = rows + 8
    size = rows + 16
    extras = blocks * size
    halves = ((1, 3), (0, 2))
    column = {j: n * slots for n, j in enumerate(halves[0] + halves[1])}

    odd = lax.rem(tile, 2) == 1
    even = jnp.logical_not(odd)
    first = lev == 0
    lone = jnp.logical_and(even, first)
    helper = jnp.logical_and(odd, first)
    feeder = jnp.logical_and(even, jnp.logical_not(first))
    second = jnp.logical_and(even, lev == 1)
    other = jnp.logical_and(odd, jnp.logical_not(first))
    even_panel = lax.rem(panel, 2) == 0
    odd_panel = jnp.logical_not(even_panel)
    has_prev, has_next = tile > 0, tile < n_tile - 1
    whole = jnp.logical_and(has_prev, has_next)
    yes = tile >= 0
    next_panel, prev_panel = lax.rem(panel + 1, n_panel), lax.rem(panel + n_panel - 1, n_panel)
    prev_tile, next_tile = jnp.maximum(tile - 1, 0), jnp.minimum(tile + 1, n_tile - 1)
    toward = [{"tile": prev_tile}, {"tile": next_tile}, {"panel": prev_panel}, {"panel": next_panel}]
    sends_to = [has_prev, has_next, yes, yes]
    comes_from = [{"tile": next_tile}, {"tile": prev_tile}, {"panel": next_panel}, {"panel": prev_panel}]
    hears = [has_next, has_prev, yes, yes]
    adds = [jnp.logical_or(jnp.logical_not(first), f) for f in (odd, odd, even, even)]

    loads = [
        pltpu.make_async_copy(src, dst, in_sem.at[i])
        for i, (src, dst) in enumerate(
            (
                (sp_hbm, sp),
                (w_hbm, w.at[lev]),
                (count_hbm, count_ref),
                (turn_hbm, turn_ref),
                (dep_hbm, dep),
                (x_hbm, x),
            )
        )
    ]
    for load in loads:
        load.start()

    barrier = pltpu.get_barrier_semaphore()

    def greet(device):
        pl.semaphore_signal(barrier, inc=1, device_id=device, device_id_type=MESH)

    @pl.when(lone)
    def _():
        greet({"tile": next_tile})

        @pl.when(odd_panel)
        def _():
            for p in (prev_panel, next_panel):
                for t in range(2):
                    greet({"panel": p, "lev": t})

    @pl.when(jnp.logical_not(lone))
    def _():
        for d in range(1, n_lev):
            greet({"lev": lax.rem(lev + d, n_lev)})
        for j in range(blocks):

            @pl.when(hears[j])
            def _(j=j):
                greet(comes_from[j])

                @pl.when(adds[j])
                def _():
                    greet({**comes_from[j], "lev": jnp.where(first, 1, 0)})

    @pl.when(helper)
    def _():
        for t in range(1, n_lev):
            greet({"tile": prev_tile, "lev": t})

        @pl.when(even_panel)
        def _():
            for p in (prev_panel, next_panel):
                for t in range(2):
                    greet({"panel": p, "tile": prev_tile, "lev": t})

        @pl.when(tile > 1)
        def _():
            greet({"tile": tile - 2})

    acc[...] = jnp.zeros_like(acc)
    for j in range(2):

        @pl.when(jnp.logical_not(hears[j]))
        def _(j=j):
            inbox[j * size : (j + 1) * size, :] = jnp.zeros((size, slots), F32)


    sent_blocks = 2 + has_prev.astype(I32) + has_next.astype(I32)
    more = jnp.where(first, n_lev - 1, 0) + jnp.where(second, 1, 0)

    def weight_copy(d, dst, sem, device):
        return pltpu.make_async_remote_copy(
            src_ref=w.at[lev],
            dst_ref=dst.at[lev],
            send_sem=w_send,
            recv_sem=sem,
            device_id=device,
            device_id_type=MESH,
        )

    def enter():
        pl.semaphore_wait(barrier, n_lev - 1 + sent_blocks * (1 + more))
        for d in (2, 3, 1):
            indirect = jnp.logical_and(even, lev == n_lev - d)

            @pl.when(indirect)
            def _(d=d):
                weight_copy(d, relay, r_recv, {"tile": next_tile, "lev": 0}).start()

            @pl.when(jnp.logical_not(indirect))
            def _(d=d):
                weight_copy(d, w, w_recv.at[lev], {"lev": lax.rem(lev + d, n_lev)}).start()

    for load in loads[:2]:
        load.wait()

    @pl.when(lone)
    def _():
        enter()

    for load in loads[2:4]:
        load.wait()

    point = [sp[j : j + 1, :] for j in range(blocks)]
    cell_high = [(p & (cells - 1)) >> shift_low for p in point]
    stencil_of = [p >> shift_cell for p in point]
    lane = lax.broadcasted_iota(I32, (1, slots), 1)
    live = [lane < count_ref[j] for j in range(blocks)]
    for j in range(blocks):
        hot[:, column[j] : column[j] + slots] = one_hot(point[j] & (LOW - 1), slots)

    def slot_weights(parts):
        lhs = []
        for t in parts:
            for i in range(per_lev):
                w4 = w[t, :, i * LOW : (i + 1) * LOW]
                b1 = w4.astype(BF16).astype(F32)
                b2 = (w4 - b1).astype(BF16).astype(F32)
                lhs.append(
                    jnp.concatenate([b1, b2, w4 - b1 - b2, jnp.zeros_like(w4)], axis=0).astype(BF16)
                )
        found = jnp.dot(jnp.concatenate(lhs, axis=0), hot[...], preferred_element_type=F32)
        row16 = lax.broadcasted_iota(I32, (16, slots), 0)
        result = []
        for j in range(blocks):
            total = jnp.zeros((16, slots), F32)
            for n, t in enumerate(parts):
                for i in range(per_lev):
                    r = n * per_lev + i
                    piece = found[r * 16 : (r + 1) * 16, column[j] : column[j] + slots]
                    total = total + jnp.where(cell_high[j] == t * per_lev + i, piece, 0.0)
            own = (row16 & (stencil - 1)) == stencil_of[j]
            weight = jnp.sum(jnp.where(own, total, 0.0), axis=0, keepdims=True)
            result.append(jnp.where(live[j], weight, 0.0))
        return result

    aslant = jnp.logical_and(lone, odd_panel)

    def ahead(j, moved):
        if j >= 2:
            return {**toward[j], "tile": tile + moved}
        return {"tile": toward[j]["tile"] + moved}

    def block_copy(j):
        moved = jnp.where(helper, 1, 0) if j == 1 else (jnp.where(aslant, 1, 0) if j >= 2 else 0)
        at = j * size if j == 0 else pl.multiple_of(j * size + moved * (blocks * (size + 8) - size), 8)
        return pltpu.make_async_remote_copy(
            src_ref=pay.at[j],
            dst_ref=inbox.at[pl.ds(at, size)],
            send_sem=p_send,
            recv_sem=p_recv.at[jnp.where(moved == 1, 2, j % 2)],
            device_id=ahead(j, moved),
            device_id_type=MESH,
        )

    def extra_copy(j, level):
        moved = jnp.where(jnp.logical_and(second, odd_panel), 1, 0) if level == 0 and j >= 2 else 0
        return pltpu.make_async_remote_copy(
            src_ref=mine.at[j] if level else pay.at[j, pl.ds(at_slot, 8)],
            dst_ref=inbox.at[pl.ds(extras + 8 * j, 8)],
            send_sem=e_send,
            recv_sem=p_recv.at[jnp.where(moved == 1, 2, j % 2)],
            device_id={**ahead(j, moved), "lev": level},
            device_id_type=MESH,
        )

    def send_blocks(which=(1, 0, 2, 3)):
        for j in which:

            @pl.when(sends_to[j])
            def _(j=j):
                block_copy(j).start()

    for j, weight in enumerate(slot_weights([lev])):
        pay[j, at_slot:, :] = jnp.broadcast_to(weight, (8, slots))
        mine[j] = jnp.broadcast_to(weight, (8, slots))

    def send_mine():
        for t in range(1, n_lev):
            for j in (1, 0, 2, 3):

                @pl.when(sends_to[j])
                def _(j=j, t=t):
                    extra_copy(j, t).start()

    @pl.when(lone)
    def _():
        send_mine()

    for load in loads[4:]:
        load.wait()

    height = 2 * rows + 16
    for g in range(groups):
        part = x[:, :, g * LOW : (g + 1) * LOW].reshape(rows, LOW)
        d4 = dep[:, g * LOW : (g + 1) * LOW]
        d8 = jnp.concatenate([d4 >> shift_low, d4 & (LOW - 1)], axis=0).astype(F32)
        d16 = jnp.concatenate([d8, jnp.zeros((8, LOW), F32)], axis=0).astype(BF16)
        glhs[g * height : g * height + 2 * rows, :] = split_rows(part)
        glhs[g * height + 2 * rows : (g + 1) * height, :] = d16
    row8 = lax.broadcasted_iota(I32, (8, slots), 0)
    some = groups // 2
    for n, pair in enumerate(halves):
        found = [
            jnp.dot(
                glhs[m * some * height : (m + 1) * some * height, :],
                hot[:, n * LOW : (n + 1) * LOW],
                preferred_element_type=F32,
            )
            for m in range(2)
        ]
        for i, j in enumerate(pair):
            total = jnp.zeros((height, slots), F32)
            for g in range(groups):
                top = (g % some) * height
                piece = found[g // some][top : top + height, i * slots : (i + 1) * slots]
                total = total + jnp.where(cell_high[j] == g, piece, 0.0)
            value = total[:rows] + total[rows : 2 * rows]
            if j >= 2:
                code = turn_ref[j - 2]
                cosine = jnp.where(code == 0, 1.0, 0.0) - jnp.where(code == 2, 1.0, 0.0)
                sine = jnp.where(code == 1, 1.0, 0.0) - jnp.where(code == 3, 1.0, 0.0)
                zonal, merid = value[:levels], value[levels : 2 * levels]
                value = jnp.concatenate(
                    [
                        cosine * zonal + sine * merid,
                        cosine * merid - sine * zonal,
                        value[2 * levels :],
                    ],
                    axis=0,
                )
            scale = jnp.where(row8 < stencil, float(LOW), 1.0)
            own = (row8 & (stencil - 1)) == stencil_of[j]
            target = jnp.sum(
                jnp.where(own, total[2 * rows : 2 * rows + 8] * scale, 0.0), axis=0, keepdims=True
            )
            pay[j, 0:rows, :] = value
            pay[j, rows:at_slot, :] = jnp.broadcast_to(target, (8, slots))

        @pl.when(lone)
        def _(pair=pair):
            send_blocks(pair)

    number = lax.broadcasted_iota(I32, (stencil * groups, slots), 0)
    marks = [
        jnp.where((number == (point[j] >> shift_low)) & live[j], 1.0, 0.0).astype(BF16)
        for j in halves[0] + halves[1]
    ]
    sent[...] = times_transposed(jnp.concatenate(marks, axis=1), hot[...])

    def segment(t):
        result = None
        for i in range(per_lev):
            at = pl.ds(pl.multiple_of(t * share + i * LOW, LOW), LOW)
            part = x[:, :, at].reshape(rows, LOW)
            for k in range(stencil):
                weight = w[t, k : k + 1, i * LOW : (i + 1) * LOW]
                landing = dep[k : k + 1, at]
                gone = sent[pl.ds(k * groups + t * per_lev + i, 1), :]
                high = jnp.where(gone > 0.5, groups, landing >> shift_low)
                term = spread(part * weight, high, landing & (LOW - 1), groups)
                result = term if result is None else result + term
        return result

    order = [
        lev,
        jnp.where(first, 1, 1 + lax.rem(lev, 3)),
        jnp.where(first, 2, 1 + lax.rem(lev + 1, 3)),
        jnp.where(first, 3, 0),
    ]

    def await_bytes(ref, sem):
        pltpu.make_async_copy(ref, ref, sem).wait()

    def add_weights(parts):
        weights = slot_weights(parts)
        for j in range(blocks):
            pay[j, at_slot:, :] += jnp.broadcast_to(weights[j], (8, slots))
        send_blocks()

    def to_lone(src, dst, send_sem, recv_sem):
        return pltpu.make_async_remote_copy(
            src_ref=src,
            dst_ref=dst,
            send_sem=send_sem,
            recv_sem=recv_sem,
            device_id={"tile": prev_tile},
            device_id_type=MESH,
        )

    others = pl.ds(1, n_lev - 1)
    relay_copy = to_lone(relay.at[others], w.at[others], z_send.at[0], w_recv.at[0])
    aside = blocks * (size + 8)
    pass_on = [
        to_lone(
            inbox.at[pl.ds(aside + (j - 1) * size, size)],
            inbox.at[pl.ds(j * size, size)],
            z_send.at[1],
            p_recv.at[j % 2],
        )
        for j in range(1, blocks)
    ]
    pass_extra = [
        to_lone(
            inbox.at[pl.ds(extras + 8 * j, 8)],
            inbox.at[pl.ds(extras + 8 * j, 8)],
            z_send.at[1],
            p_recv.at[j % 2],
        )
        for j in (2, 3)
    ]
    passed = [
        (functools.reduce(jnp.logical_and, (helper, *case)), rows_passed)
        for case, rows_passed in (
            ((even_panel, tile > 1), 3 * size + 16),
            ((even_panel, tile == 1), 2 * size + 16),
            ((odd_panel, tile > 1), size),
        )
    ]

    def both(*conditions):
        return functools.reduce(jnp.logical_and, conditions)

    soon = both(feeder, even_panel, lax.rem(tile, 4) == 0)

    def step(i, carry):
        @pl.when(i == jnp.where(helper, 3, jnp.where(other, 1, jnp.where(feeder, 0, -1))))
        def _():
            enter()

        when = (
            jnp.where(lone, -1, 1),
            jnp.where(lone, -1, jnp.where(feeder, 1, 2)),
            jnp.where(lone, -1, jnp.where(soon, 4, 3)),
        )
        for n in range(2):

            @pl.when(i == when[n])
            def _(n=n):
                await_bytes(w.at[order[n + 1]], w_recv.at[order[n + 1]])

        @pl.when(both(helper, i == 3))
        def _():
            send_mine()
            await_bytes(w.at[order[3]], w_recv.at[order[3]])
            add_weights(order[1:])

        @pl.when(both(jnp.logical_not(first), i == when[1]))
        def _():
            add_weights(order[1:3])

            @pl.when(second)
            def _():
                for j in range(blocks):

                    @pl.when(sends_to[j])
                    def _(j=j):
                        extra_copy(j, 0).start()

        @pl.when(both(helper, i == 3))
        def _():
            await_bytes(relay.at[others], r_recv)
            relay_copy.start()

        @pl.when(both(lone, i == 1))
        def _():
            await_bytes(w.at[others], w_recv.at[0])

        for case, n in passed:

            @pl.when(both(case, i == 4))
            def _(n=n):
                await_bytes(inbox.at[pl.ds(0, n)], p_recv.at[2])

        @pl.when(both(helper, i == 4))
        def _():
            @pl.when(tile > 1)
            def _():
                pass_on[0].start()

            @pl.when(even_panel)
            def _():
                for copy in pass_on[1:] + pass_extra:
                    copy.start()

        arriving = i == jnp.where(soon, 3, 4)

        @pl.when(jnp.logical_not(arriving))
        def _():
            k = jnp.minimum(i, 3)
            t = jnp.where(
                k == 0, order[0], jnp.where(k == 1, order[1], jnp.where(k == 2, order[2], order[3]))
            )
            @pl.when(both(jnp.logical_not(first), i == when[2]))
            def _():
                await_bytes(w.at[0], w_recv.at[0])

            acc[...] += segment(t)

        @pl.when(arriving)
        def _():
            await_bytes(w.at[others], w_send)
            for n, edge in ((blocks, whole), (blocks - 1, jnp.logical_not(whole))):

                @pl.when(edge)
                def _(n=n):
                    await_bytes(pay.at[pl.ds(0, n)], p_send)

                for role, times in ((first, n_lev - 1), (second, 1)):

                    @pl.when(both(role, edge))
                    def _(n=n, times=times):
                        await_bytes(inbox.at[pl.ds(0, 8 * n * times)], e_send)

            @pl.when(helper)
            def _():
                await_bytes(relay.at[others], z_send.at[0])

            for half, here in ((0, has_next), (1, has_prev)):
                there = jnp.logical_not(here)
                for case, n in (
                    (both(here, first), 2 * size + 8),
                    (both(here, jnp.logical_not(first)), 2 * size + 16),
                    (both(there, odd, first), size),
                    (both(there, jnp.logical_or(even, jnp.logical_not(first))), size + 8),
                ):

                    @pl.when(case)
                    def _(n=n, half=half):
                        await_bytes(inbox.at[pl.ds(0, n)], p_recv.at[half])

                for j in (half, half + 2):

                    @pl.when(jnp.logical_and(hears[j], adds[j]))
                    def _(j=j):
                        inbox[j * size + at_slot : (j + 1) * size, :] += inbox[
                            extras + 8 * j : extras + 8 * (j + 1), :
                        ]

            result = acc[...]
            for pair in halves:
                value = jnp.concatenate(
                    [
                        inbox[j * size : j * size + rows, :]
                        * inbox[j * size + at_slot : j * size + at_slot + 1, :]
                        for j in pair
                    ],
                    axis=1,
                )
                landing = jnp.concatenate(
                    [inbox[j * size + rows : j * size + rows + 1, :] for j in pair], axis=1
                ).astype(I32)
                result = result + spread(value, landing >> shift_low, landing & (LOW - 1), groups)
            acc[...] = result

        return carry

    lax.fori_loop(0, 5, step, 0)

    result = acc
    for g in range(groups):
        top = g * 2 * rows
        out_ref[:, :, g * LOW : (g + 1) * LOW] = (
            result[top : top + rows, :] + result[top + rows : top + 2 * rows, :]
        ).reshape(fields, levels, LOW)

    for case, n in passed:

        @pl.when(case)
        def _(n=n):
            await_bytes(inbox.at[pl.ds(0, n)], z_send.at[1])


def scoped(sizes, *refs):
    dma = pltpu.SemaphoreType.DMA
    pl.run_scoped(functools.partial(kernel, sizes, *refs), dma((6,)), dma, dma, dma, dma((2,)))


def body(sizes, adjoint_new, weights, departure, send_point, block_count, rotation):
    fields, levels, cells = adjoint_new.shape
    stencil = departure.shape[0]
    blocks, slots = send_point.shape
    rows = fields * levels
    groups = cells // LOW
    n_lev = sizes[2]
    hbm = pl.BlockSpec(memory_space=pltpu.HBM)
    args = (adjoint_new, weights, departure, send_point, block_count.reshape(-1), rotation.reshape(-1))
    return pl.pallas_call(
        functools.partial(scoped, sizes),
        out_shape=pltpu.VMEM(adjoint_new.shape, F32),
        in_specs=[hbm] * len(args),
        out_specs=pl.BlockSpec(memory_space=pltpu.VMEM),
        scratch_shapes=[
            pltpu.SMEM((blocks,), I32),
            pltpu.SMEM((rotation.shape[0],), I32),
            pltpu.VMEM((fields, levels, cells), F32),
            pltpu.VMEM((n_lev, stencil, cells // n_lev), F32),
            pltpu.VMEM((n_lev, stencil, cells // n_lev), F32),
            pltpu.VMEM((stencil, cells), I32),
            pltpu.VMEM((blocks, slots), I32),
            pltpu.VMEM((LOW, blocks * slots), BF16),
            pltpu.VMEM((groups * (2 * rows + 16), LOW), BF16),
            pltpu.VMEM((stencil * groups, LOW), F32),
            pltpu.VMEM((groups * 2 * rows, LOW), F32),
            pltpu.VMEM((blocks, rows + 16, slots), F32),
            pltpu.VMEM((blocks, 8, slots), F32),
            pltpu.VMEM((blocks * (rows + 24) + 3 * (rows + 16), slots), F32),
            pltpu.SemaphoreType.DMA((n_lev,)),
            pltpu.SemaphoreType.DMA,
            pltpu.SemaphoreType.DMA((3,)),
        ],
        compiler_params=pltpu.CompilerParams(
            collective_id=0, has_side_effects=True, vmem_limit_bytes=16 * 1024 * 1024
        ),
    )(*(pltpu.with_memory_space_constraint(a, pltpu.HBM) for a in args))


def solution(mesh):
    sizes = tuple(mesh.shape[a] for a in ("panel", "tile", "lev"))
    return jax.shard_map(
        functools.partial(body, sizes),
        mesh=mesh,
        in_specs=(
            P(None, "lev", ("panel", "tile")),
            P(None, ("panel", "tile", "lev")),
            P(None, ("panel", "tile")),
            P(None, ("panel", "tile")),
            P(None, ("panel", "tile")),
            P(None, ("panel", "tile")),
        ),
        out_specs=P(None, "lev", ("panel", "tile")),
        check_vma=False,
    )
```

```python
import functools

import jax
import jax.numpy as jnp
from jax import lax
from jax.experimental import pallas as pl
from jax.experimental.pallas import tpu as pltpu
from jax.sharding import PartitionSpec as P

MESH = pl.DeviceIdType.MESH
LOW = 256
F32, BF16, I32 = jnp.float32, jnp.bfloat16, jnp.int32


def split_rows(value):
    high = value.astype(BF16).astype(F32)
    return jnp.concatenate([high, value - high], axis=0).astype(BF16)


def one_hot(low, columns):
    rows = lax.broadcasted_iota(I32, (LOW, columns), 0)
    return jnp.where(rows == low, 1.0, 0.0).astype(BF16)


def times_transposed(lhs, rhs):
    return lax.dot_general(lhs, rhs, (((1,), (1,)), ((), ())), preferred_element_type=F32)


def spread(value, target_high, target_low, groups):
    parts = split_rows(value)
    copies = parts.shape[0] // 16
    high = jnp.broadcast_to(target_high, (16, LOW))
    lhs = []
    for g in range(groups):
        mask = jnp.where(high == g, 1.0, 0.0).astype(BF16)
        lhs.append(parts * jnp.concatenate([mask] * copies, axis=0))
    return times_transposed(jnp.concatenate(lhs, axis=0), one_hot(target_low, LOW))


def kernel(
    sizes,
    x_hbm,
    w_hbm,
    dep_hbm,
    sp_hbm,
    count_hbm,
    turn_hbm,
    out_ref,
    count_ref,
    turn_ref,
    x,
    w,
    relay,
    dep,
    sp,
    hot,
    glhs,
    sent,
    acc,
    pay,
    mine,
    inbox,
    w_recv,
    r_recv,
    p_recv,
    in_sem,
    w_send,
    p_send,
    e_send,
    z_send,
):
    n_panel, n_tile, n_lev = sizes
    fields, levels, cells = x.shape
    stencil = dep.shape[0]
    blocks, slots = sp.shape
    rows = fields * levels
    groups = cells // LOW
    share = cells // n_lev
    per_lev = share // LOW
    panel, tile, lev = (lax.axis_index(a) for a in ("panel", "tile", "lev"))
    shift_cell = cells.bit_length() - 1
    shift_low = LOW.bit_length() - 1
    at_slot = rows + 8
    size = rows + 16
    extras = blocks * size
    halves = ((1, 3), (0, 2))
    column = {j: n * slots for n, j in enumerate(halves[0] + halves[1])}

    odd = lax.rem(tile, 2) == 1
    even = jnp.logical_not(odd)
    first = lev == 0
    lone = jnp.logical_and(even, first)
    helper = jnp.logical_and(odd, first)
    feeder = jnp.logical_and(even, jnp.logical_not(first))
    second = jnp.logical_and(even, lev == 1)
    other = jnp.logical_and(odd, jnp.logical_not(first))
    even_panel = lax.rem(panel, 2) == 0
    odd_panel = jnp.logical_not(even_panel)
    has_prev, has_next = tile > 0, tile < n_tile - 1
    whole = jnp.logical_and(has_prev, has_next)
    yes = tile >= 0
    next_panel, prev_panel = lax.rem(panel + 1, n_panel), lax.rem(panel + n_panel - 1, n_panel)
    prev_tile, next_tile = jnp.maximum(tile - 1, 0), jnp.minimum(tile + 1, n_tile - 1)
    toward = [{"tile": prev_tile}, {"tile": next_tile}, {"panel": prev_panel}, {"panel": next_panel}]
    sends_to = [has_prev, has_next, yes, yes]
    comes_from = [{"tile": next_tile}, {"tile": prev_tile}, {"panel": next_panel}, {"panel": prev_panel}]
    hears = [has_next, has_prev, yes, yes]
    adds = [jnp.logical_or(jnp.logical_not(first), f) for f in (odd, odd, even, even)]

    loads = [
        pltpu.make_async_copy(src, dst, in_sem.at[i])
        for i, (src, dst) in enumerate(
            (
                (sp_hbm, sp),
                (w_hbm, w.at[lev]),
                (count_hbm, count_ref),
                (turn_hbm, turn_ref),
                (dep_hbm, dep),
                (x_hbm, x),
            )
        )
    ]
    for load in loads:
        load.start()

    barrier = pltpu.get_barrier_semaphore()

    def greet(device):
        pl.semaphore_signal(barrier, inc=1, device_id=device, device_id_type=MESH)

    @pl.when(lone)
    def _():
        greet({"tile": next_tile})

        @pl.when(odd_panel)
        def _():
            for p in (prev_panel, next_panel):
                for t in range(2):
                    greet({"panel": p, "lev": t})

    @pl.when(jnp.logical_not(lone))
    def _():
        for d in range(1, n_lev):
            greet({"lev": lax.rem(lev + d, n_lev)})
        for j in range(blocks):

            @pl.when(hears[j])
            def _(j=j):
                greet(comes_from[j])

                @pl.when(adds[j])
                def _():
                    greet({**comes_from[j], "lev": jnp.where(first, 1, 0)})

    @pl.when(helper)
    def _():
        for t in range(1, n_lev):
            greet({"tile": prev_tile, "lev": t})

        @pl.when(even_panel)
        def _():
            for p in (prev_panel, next_panel):
                for t in range(2):
                    greet({"panel": p, "tile": prev_tile, "lev": t})

        @pl.when(tile > 1)
        def _():
            greet({"tile": tile - 2})

    acc[...] = jnp.zeros_like(acc)
    for j in range(2):

        @pl.when(jnp.logical_not(hears[j]))
        def _(j=j):
            inbox[j * size : (j + 1) * size, :] = jnp.zeros((size, slots), F32)


    sent_blocks = 2 + has_prev.astype(I32) + has_next.astype(I32)
    more = jnp.where(first, n_lev - 1, 0) + jnp.where(second, 1, 0)

    def weight_copy(d, dst, sem, device):
        return pltpu.make_async_remote_copy(
            src_ref=w.at[lev],
            dst_ref=dst.at[lev],
            send_sem=w_send,
            recv_sem=sem,
            device_id=device,
            device_id_type=MESH,
        )

    def enter():
        pl.semaphore_wait(barrier, n_lev - 1 + sent_blocks * (1 + more))
        for d in (2, 3, 1):
            indirect = jnp.logical_and(even, lev == n_lev - d)

            @pl.when(indirect)
            def _(d=d):
                weight_copy(d, relay, r_recv, {"tile": next_tile, "lev": 0}).start()

            @pl.when(jnp.logical_not(indirect))
            def _(d=d):
                weight_copy(d, w, w_recv.at[lev], {"lev": lax.rem(lev + d, n_lev)}).start()

    for load in loads[:2]:
        load.wait()

    @pl.when(lone)
    def _():
        enter()

    for load in loads[2:4]:
        load.wait()

    point = [sp[j : j + 1, :] for j in range(blocks)]
    cell_high = [(p & (cells - 1)) >> shift_low for p in point]
    stencil_of = [p >> shift_cell for p in point]
    lane = lax.broadcasted_iota(I32, (1, slots), 1)
    live = [lane < count_ref[j] for j in range(blocks)]
    for j in range(blocks):
        hot[:, column[j] : column[j] + slots] = one_hot(point[j] & (LOW - 1), slots)

    def slot_weights(parts):
        lhs = []
        for t in parts:
            for i in range(per_lev):
                w4 = w[t, :, i * LOW : (i + 1) * LOW]
                b1 = w4.astype(BF16).astype(F32)
                b2 = (w4 - b1).astype(BF16).astype(F32)
                lhs.append(
                    jnp.concatenate([b1, b2, w4 - b1 - b2, jnp.zeros_like(w4)], axis=0).astype(BF16)
                )
        found = jnp.dot(jnp.concatenate(lhs, axis=0), hot[...], preferred_element_type=F32)
        row16 = lax.broadcasted_iota(I32, (16, slots), 0)
        result = []
        for j in range(blocks):
            total = jnp.zeros((16, slots), F32)
            for n, t in enumerate(parts):
                for i in range(per_lev):
                    r = n * per_lev + i
                    piece = found[r * 16 : (r + 1) * 16, column[j] : column[j] + slots]
                    total = total + jnp.where(cell_high[j] == t * per_lev + i, piece, 0.0)
            own = (row16 & (stencil - 1)) == stencil_of[j]
            weight = jnp.sum(jnp.where(own, total, 0.0), axis=0, keepdims=True)
            result.append(jnp.where(live[j], weight, 0.0))
        return result

    aslant = jnp.logical_and(lone, odd_panel)

    def ahead(j, moved):
        if j >= 2:
            return {**toward[j], "tile": tile + moved}
        return {"tile": toward[j]["tile"] + moved}

    def block_copy(j):
        moved = jnp.where(helper, 1, 0) if j == 1 else (jnp.where(aslant, 1, 0) if j >= 2 else 0)
        at = j * size if j == 0 else pl.multiple_of(j * size + moved * (blocks * (size + 8) - size), 8)
        return pltpu.make_async_remote_copy(
            src_ref=pay.at[j],
            dst_ref=inbox.at[pl.ds(at, size)],
            send_sem=p_send,
            recv_sem=p_recv.at[jnp.where(moved == 1, 2, j % 2)],
            device_id=ahead(j, moved),
            device_id_type=MESH,
        )

    def extra_copy(j, level):
        moved = jnp.where(jnp.logical_and(second, odd_panel), 1, 0) if level == 0 and j >= 2 else 0
        return pltpu.make_async_remote_copy(
            src_ref=mine.at[j] if level else pay.at[j, pl.ds(at_slot, 8)],
            dst_ref=inbox.at[pl.ds(extras + 8 * j, 8)],
            send_sem=e_send,
            recv_sem=p_recv.at[jnp.where(moved == 1, 2, j % 2)],
            device_id={**ahead(j, moved), "lev": level},
            device_id_type=MESH,
        )

    def send_blocks(which=(1, 0, 2, 3)):
        for j in which:

            @pl.when(sends_to[j])
            def _(j=j):
                block_copy(j).start()

    for load in loads[4:]:
        load.wait()

    for j, weight in enumerate(slot_weights([lev])):
        pay[j, at_slot:, :] = jnp.broadcast_to(weight, (8, slots))
        mine[j] = jnp.broadcast_to(weight, (8, slots))

    def send_mine():
        for t in range(1, n_lev):
            for j in (1, 0, 2, 3):

                @pl.when(sends_to[j])
                def _(j=j, t=t):
                    extra_copy(j, t).start()

    height = 2 * rows + 16
    for g in range(groups):
        part = x[:, :, g * LOW : (g + 1) * LOW].reshape(rows, LOW)
        d4 = dep[:, g * LOW : (g + 1) * LOW]
        d8 = jnp.concatenate([d4 >> shift_low, d4 & (LOW - 1)], axis=0).astype(F32)
        d16 = jnp.concatenate([d8, jnp.zeros((8, LOW), F32)], axis=0).astype(BF16)
        glhs[g * height : g * height + 2 * rows, :] = split_rows(part)
        glhs[g * height + 2 * rows : (g + 1) * height, :] = d16
    row8 = lax.broadcasted_iota(I32, (8, slots), 0)
    some = groups // 2
    for n, pair in enumerate(halves):
        found = [
            jnp.dot(
                glhs[m * some * height : (m + 1) * some * height, :],
                hot[:, n * LOW : (n + 1) * LOW],
                preferred_element_type=F32,
            )
            for m in range(2)
        ]
        for i, j in enumerate(pair):
            total = jnp.zeros((height, slots), F32)
            for g in range(groups):
                top = (g % some) * height
                piece = found[g // some][top : top + height, i * slots : (i + 1) * slots]
                total = total + jnp.where(cell_high[j] == g, piece, 0.0)
            value = total[:rows] + total[rows : 2 * rows]
            if j >= 2:
                code = turn_ref[j - 2]
                cosine = jnp.where(code == 0, 1.0, 0.0) - jnp.where(code == 2, 1.0, 0.0)
                sine = jnp.where(code == 1, 1.0, 0.0) - jnp.where(code == 3, 1.0, 0.0)
                zonal, merid = value[:levels], value[levels : 2 * levels]
                value = jnp.concatenate(
                    [
                        cosine * zonal + sine * merid,
                        cosine * merid - sine * zonal,
                        value[2 * levels :],
                    ],
                    axis=0,
                )
            scale = jnp.where(row8 < stencil, float(LOW), 1.0)
            own = (row8 & (stencil - 1)) == stencil_of[j]
            target = jnp.sum(
                jnp.where(own, total[2 * rows : 2 * rows + 8] * scale, 0.0), axis=0, keepdims=True
            )
            pay[j, 0:rows, :] = value
            pay[j, rows:at_slot, :] = jnp.broadcast_to(target, (8, slots))

        @pl.when(lone)
        def _(n=n, pair=pair):
            send_blocks(pair)
            if n == 0:
                send_mine()

    number = lax.broadcasted_iota(I32, (stencil * groups, slots), 0)
    marks = [
        jnp.where((number == (point[j] >> shift_low)) & live[j], 1.0, 0.0).astype(BF16)
        for j in halves[0] + halves[1]
    ]
    sent[...] = times_transposed(jnp.concatenate(marks, axis=1), hot[...])

    def segment(t):
        result = None
        for i in range(per_lev):
            at = pl.ds(pl.multiple_of(t * share + i * LOW, LOW), LOW)
            part = x[:, :, at].reshape(rows, LOW)
            for k in range(stencil):
                weight = w[t, k : k + 1, i * LOW : (i + 1) * LOW]
                landing = dep[k : k + 1, at]
                gone = sent[pl.ds(k * groups + t * per_lev + i, 1), :]
                high = jnp.where(gone > 0.5, groups, landing >> shift_low)
                term = spread(part * weight, high, landing & (LOW - 1), groups)
                result = term if result is None else result + term
        return result

    order = [
        lev,
        jnp.where(first, 1, 1 + lax.rem(lev, 3)),
        jnp.where(first, 2, 1 + lax.rem(lev + 1, 3)),
        jnp.where(first, 3, 0),
    ]

    def await_bytes(ref, sem):
        pltpu.make_async_copy(ref, ref, sem).wait()

    def add_weights(parts):
        weights = slot_weights(parts)
        for j in range(blocks):
            pay[j, at_slot:, :] += jnp.broadcast_to(weights[j], (8, slots))
        send_blocks()

    def to_lone(src, dst, send_sem, recv_sem):
        return pltpu.make_async_remote_copy(
            src_ref=src,
            dst_ref=dst,
            send_sem=send_sem,
            recv_sem=recv_sem,
            device_id={"tile": prev_tile},
            device_id_type=MESH,
        )

    others = pl.ds(1, n_lev - 1)
    relay_copy = to_lone(relay.at[others], w.at[others], z_send.at[0], w_recv.at[0])
    aside = blocks * (size + 8)
    pass_on = [
        to_lone(
            inbox.at[pl.ds(aside + (j - 1) * size, size)],
            inbox.at[pl.ds(j * size, size)],
            z_send.at[1],
            p_recv.at[j % 2],
        )
        for j in range(1, blocks)
    ]
    pass_extra = [
        to_lone(
            inbox.at[pl.ds(extras + 8 * j, 8)],
            inbox.at[pl.ds(extras + 8 * j, 8)],
            z_send.at[1],
            p_recv.at[j % 2],
        )
        for j in (2, 3)
    ]
    passed = [
        (functools.reduce(jnp.logical_and, (helper, *case)), rows_passed)
        for case, rows_passed in (
            ((even_panel, tile > 1), 3 * size + 16),
            ((even_panel, tile == 1), 2 * size + 16),
            ((odd_panel, tile > 1), size),
        )
    ]

    def both(*conditions):
        return functools.reduce(jnp.logical_and, conditions)

    soon = both(feeder, even_panel, lax.rem(tile, 4) == 0)

    def step(i, carry):
        @pl.when(i == jnp.where(helper, 3, jnp.where(other, 1, jnp.where(feeder, 0, -1))))
        def _():
            enter()

        when = (
            jnp.where(lone, -1, 1),
            jnp.where(lone, -1, jnp.where(feeder, 1, 2)),
            jnp.where(lone, -1, jnp.where(soon, 4, 3)),
        )
        for n in range(2):

            @pl.when(i == when[n])
            def _(n=n):
                await_bytes(w.at[order[n + 1]], w_recv.at[order[n + 1]])

        @pl.when(both(helper, i == 3))
        def _():
            send_mine()
            await_bytes(w.at[order[3]], w_recv.at[order[3]])
            add_weights(order[1:])

        @pl.when(both(jnp.logical_not(first), i == when[1]))
        def _():
            add_weights(order[1:3])

            @pl.when(second)
            def _():
                for j in range(blocks):

                    @pl.when(sends_to[j])
                    def _(j=j):
                        extra_copy(j, 0).start()

        @pl.when(both(helper, i == 3))
        def _():
            await_bytes(relay.at[others], r_recv)
            relay_copy.start()

        @pl.when(both(lone, i == 1))
        def _():
            await_bytes(w.at[others], w_recv.at[0])

        for case, n in passed:

            @pl.when(both(case, i == 4))
            def _(n=n):
                await_bytes(inbox.at[pl.ds(0, n)], p_recv.at[2])

        @pl.when(both(helper, i == 4))
        def _():
            @pl.when(tile > 1)
            def _():
                pass_on[0].start()

            @pl.when(even_panel)
            def _():
                for copy in pass_on[1:] + pass_extra:
                    copy.start()

        arriving = i == jnp.where(soon, 3, 4)

        @pl.when(jnp.logical_not(arriving))
        def _():
            k = jnp.minimum(i, 3)
            t = jnp.where(
                k == 0, order[0], jnp.where(k == 1, order[1], jnp.where(k == 2, order[2], order[3]))
            )
            @pl.when(both(jnp.logical_not(first), i == when[2]))
            def _():
                await_bytes(w.at[0], w_recv.at[0])

            acc[...] += segment(t)

        @pl.when(arriving)
        def _():
            await_bytes(w.at[others], w_send)
            for n, edge in ((blocks, whole), (blocks - 1, jnp.logical_not(whole))):

                @pl.when(edge)
                def _(n=n):
                    await_bytes(pay.at[pl.ds(0, n)], p_send)

                for role, times in ((first, n_lev - 1), (second, 1)):

                    @pl.when(both(role, edge))
                    def _(n=n, times=times):
                        await_bytes(inbox.at[pl.ds(0, 8 * n * times)], e_send)

            @pl.when(helper)
            def _():
                await_bytes(relay.at[others], z_send.at[0])

            for half, here in ((0, has_next), (1, has_prev)):
                there = jnp.logical_not(here)
                for case, n in (
                    (both(here, first), 2 * size + 8),
                    (both(here, jnp.logical_not(first)), 2 * size + 16),
                    (both(there, odd, first), size),
                    (both(there, jnp.logical_or(even, jnp.logical_not(first))), size + 8),
                ):

                    @pl.when(case)
                    def _(n=n, half=half):
                        await_bytes(inbox.at[pl.ds(0, n)], p_recv.at[half])

                for j in (half, half + 2):

                    @pl.when(jnp.logical_and(hears[j], adds[j]))
                    def _(j=j):
                        inbox[j * size + at_slot : (j + 1) * size, :] += inbox[
                            extras + 8 * j : extras + 8 * (j + 1), :
                        ]

            result = acc[...]
            for pair in halves:
                value = jnp.concatenate(
                    [
                        inbox[j * size : j * size + rows, :]
                        * inbox[j * size + at_slot : j * size + at_slot + 1, :]
                        for j in pair
                    ],
                    axis=1,
                )
                landing = jnp.concatenate(
                    [inbox[j * size + rows : j * size + rows + 1, :] for j in pair], axis=1
                ).astype(I32)
                result = result + spread(value, landing >> shift_low, landing & (LOW - 1), groups)
            acc[...] = result

        return carry

    lax.fori_loop(0, 5, step, 0)

    result = acc
    for g in range(groups):
        top = g * 2 * rows
        out_ref[:, :, g * LOW : (g + 1) * LOW] = (
            result[top : top + rows, :] + result[top + rows : top + 2 * rows, :]
        ).reshape(fields, levels, LOW)

    for case, n in passed:

        @pl.when(case)
        def _(n=n):
            await_bytes(inbox.at[pl.ds(0, n)], z_send.at[1])


def scoped(sizes, *refs):
    dma = pltpu.SemaphoreType.DMA
    pl.run_scoped(functools.partial(kernel, sizes, *refs), dma((6,)), dma, dma, dma, dma((2,)))


def body(sizes, adjoint_new, weights, departure, send_point, block_count, rotation):
    fields, levels, cells = adjoint_new.shape
    stencil = departure.shape[0]
    blocks, slots = send_point.shape
    rows = fields * levels
    groups = cells // LOW
    n_lev = sizes[2]
    hbm = pl.BlockSpec(memory_space=pltpu.HBM)
    args = (adjoint_new, weights, departure, send_point, block_count.reshape(-1), rotation.reshape(-1))
    return pl.pallas_call(
        functools.partial(scoped, sizes),
        out_shape=pltpu.VMEM(adjoint_new.shape, F32),
        in_specs=[hbm] * len(args),
        out_specs=pl.BlockSpec(memory_space=pltpu.VMEM),
        scratch_shapes=[
            pltpu.SMEM((blocks,), I32),
            pltpu.SMEM((rotation.shape[0],), I32),
            pltpu.VMEM((fields, levels, cells), F32),
            pltpu.VMEM((n_lev, stencil, cells // n_lev), F32),
            pltpu.VMEM((n_lev, stencil, cells // n_lev), F32),
            pltpu.VMEM((stencil, cells), I32),
            pltpu.VMEM((blocks, slots), I32),
            pltpu.VMEM((LOW, blocks * slots), BF16),
            pltpu.VMEM((groups * (2 * rows + 16), LOW), BF16),
            pltpu.VMEM((stencil * groups, LOW), F32),
            pltpu.VMEM((groups * 2 * rows, LOW), F32),
            pltpu.VMEM((blocks, rows + 16, slots), F32),
            pltpu.VMEM((blocks, 8, slots), F32),
            pltpu.VMEM((blocks * (rows + 24) + 3 * (rows + 16), slots), F32),
            pltpu.SemaphoreType.DMA((n_lev,)),
            pltpu.SemaphoreType.DMA,
            pltpu.SemaphoreType.DMA((3,)),
        ],
        compiler_params=pltpu.CompilerParams(
            collective_id=0, has_side_effects=True, vmem_limit_bytes=16 * 1024 * 1024
        ),
    )(*(pltpu.with_memory_space_constraint(a, pltpu.HBM) for a in args))


def solution(mesh):
    sizes = tuple(mesh.shape[a] for a in ("panel", "tile", "lev"))
    return jax.shard_map(
        functools.partial(body, sizes),
        mesh=mesh,
        in_specs=(
            P(None, "lev", ("panel", "tile")),
            P(None, ("panel", "tile", "lev")),
            P(None, ("panel", "tile")),
            P(None, ("panel", "tile")),
            P(None, ("panel", "tile")),
            P(None, ("panel", "tile")),
        ),
        out_specs=P(None, "lev", ("panel", "tile")),
        check_vma=False,
    )
```
